128 devices in a mesh: sys: 1, aux: 64 (over z, y, x), orb: 2 (over core).
Axes of the slice: x: 4, y: 4, z: 4, core: 2. Of those that a mesh axis runs over, the one named last changes fastest.
Arguments:
- b_tensor: float32 [1280, 512, 512], P(('sys', 'aux'), 'orb')
- c_alpha: float32 [512, 105], P('sys')
- c_beta: float32 [512, 104], P('sys')
Outputs:
- output 1: float32 [512, 512], P(('sys', 'orb'), 'aux')
- output 2: float32 [512, 512], P(('sys', 'orb'), 'aux')
All inputs are finite; a program needn't handle non-finite values.
Results may differ from the reference program's by a relative error of at most 0.001.
Values are sent between devices in bfloat16 or wider.
A program may use at most 1 GiB of HBM per device.

```python
import math
import jax
import jax.numpy as jnp
from jax import lax

N = 512
NAUX = 1280
NALPHA = 105
NBETA = 104

TOP_PRECISION = lax.Precision.HIGHEST


def setup_inputs(seed: int = 0, part: int = 0) -> dict:
    pattern_count = 16
    root_key = jax.random.fold_in(jax.random.key(seed), part)
    key_noise, key_amp, key_orb, key_alpha, key_beta = jax.random.split(root_key, 5)
    amp_scale = (math.sqrt(pattern_count) / (NAUX * (NALPHA + NBETA))) ** 0.5
    raw_noise = jax.random.normal(key_noise, (NAUX, N, N), jnp.float32)
    sym_noise = (raw_noise + jnp.swapaxes(raw_noise, 1, 2)) * (0.5 * amp_scale / math.sqrt(2.0))
    amp_vals = jax.random.normal(key_amp, (NAUX,), jnp.float32) * amp_scale
    orb_pattern = jax.random.normal(key_orb, (pattern_count, N), jnp.float32)
    pattern_rows = jnp.repeat(orb_pattern, NAUX // pattern_count, axis=0)
    outer_prod = pattern_rows[:, :, None] * pattern_rows[:, None, :]
    b_tensor = sym_noise + amp_vals[:, None, None] * outer_prod
    c_alpha = jax.random.normal(key_alpha, (N, NALPHA), jnp.float32) / math.sqrt(N)
    c_beta = jax.random.normal(key_beta, (N, NBETA), jnp.float32) / math.sqrt(N)
    return {'b_tensor': b_tensor, 'c_alpha': c_alpha, 'c_beta': c_beta}


def reference(b_tensor, c_alpha, c_beta):
    b_full = b_tensor.astype(jnp.float32)
    alpha_full = c_alpha.astype(jnp.float32)
    beta_full = c_beta.astype(jnp.float32)
    dens_mat = jnp.dot(alpha_full, alpha_full.T, precision=TOP_PRECISION, preferred_element_type=jnp.float32) + jnp.dot(beta_full, beta_full.T, precision=TOP_PRECISION, preferred_element_type=jnp.float32)
    gamma_vec = jnp.einsum('qms,ms->q', b_full, dens_mat, precision=TOP_PRECISION)
    coul_mat = jnp.einsum('qmn,q->mn', b_full, gamma_vec, precision=TOP_PRECISION)

    def exchange(c_spin):
        half_tr = jnp.einsum('qml,li->qmi', b_full, c_spin, precision=TOP_PRECISION)
        return jnp.einsum('qmi,qni->mn', half_tr, half_tr, precision=TOP_PRECISION)

    return coul_mat - exchange(alpha_full), coul_mat - exchange(beta_full)
```

```python
import functools

import jax
import jax.numpy as jnp
from jax import lax
from jax.experimental import pallas as pl
from jax.experimental.pallas import tpu as pltpu
from jax.sharding import PartitionSpec as P

MESH = pl.DeviceIdType.MESH
F32 = jnp.float32
BF16 = jnp.bfloat16
NT = (((1,), (1,)), ((), ()))
ORDERS = ((2, 1, 0), (1, 0, 2), (0, 2, 1), (2, 0, 1))


def split3(value):
    high = value.astype(BF16)
    rest = value - high.astype(F32)
    mid = rest.astype(BF16)
    low = (rest - mid.astype(F32)).astype(BF16)
    return high, mid, low


def mm(a, b):
    return jnp.dot(a, b, preferred_element_type=F32)


def mm_nt(a, b):
    return lax.dot_general(a, b, NT, preferred_element_type=F32)


def kernel(n_q, rows, b_ref, ca_ref, cb_ref, o_ref, b_v, c_f, c_s, t_f, t_r, own, oth, j_acc, y_acc, z_acc,
           p_buf, r1, s1, r2, s2, r3, b_sem, t_send, t_recv, ph_send, ph_recv):
    pairs = n_q // 2
    half = rows // 2
    aux = lax.axis_index("aux")
    orb = lax.axis_index("orb")
    coords = (aux // 16, lax.rem(aux // 4, 4), lax.rem(aux, 4))
    strides = (16, 4, 1)
    partner = {"aux": aux, "orb": 1 - orb}

    def peer(axis, dist):
        target = lax.rem(coords[axis] + dist, 4)
        return {"aux": aux + (target - coords[axis]) * strides[axis], "orb": orb}, target

    def b_copy(q):
        return pltpu.make_async_copy(b_ref.at[q], b_v.at[q], b_sem.at[q])

    for q in range(n_q):
        b_copy(q).start()

    barrier = pltpu.get_barrier_semaphore()
    pl.semaphore_signal(barrier, inc=1, device_id=partner, device_id_type=MESH)
    for axis in range(3):
        for dist in (1, 2, 3):
            pl.semaphore_signal(barrier, inc=1, device_id=peer(axis, dist)[0], device_id_type=MESH)

    c_f[...] = jnp.zeros_like(c_f)
    c_f[:, 0:ca_ref.shape[1]] = ca_ref[...]
    c_f[:, 128:128 + cb_ref.shape[1]] = cb_ref[...]
    for k, part in enumerate(split3(c_f[...])):
        c_s[k] = part
    j_acc[...] = jnp.zeros_like(j_acc)
    y_acc[...] = jnp.zeros_like(y_acc)
    z_acc[...] = jnp.zeros_like(z_acc)
    own_row = pl.multiple_of(orb * half, half)
    oth_row = pl.multiple_of((1 - orb) * half, half)

    def t_copy(p):
        block = pl.ds(2 * p, 2)
        return pltpu.make_async_remote_copy(
            src_ref=t_f.at[block], dst_ref=t_r.at[block], send_sem=t_send.at[p], recv_sem=t_recv.at[p],
            device_id=partner, device_id_type=MESH)

    def t_step(p):
        for e in range(2):
            q = 2 * p + e
            b_copy(q).wait()
        for e in range(2):
            q = 2 * p + e
            h, m, l = split3(b_v[q])
            t = (mm(h, c_s[0]) + mm(m, c_s[0]) + mm(l, c_s[0]) + mm(h, c_s[1]) + mm(m, c_s[1]) + mm(h, c_s[2]))
            t_f[q] = t
            for k, part in enumerate(split3(t)):
                for s in range(2):
                    own[p, k, s, :, e * 128:(e + 1) * 128] = part[:, s * 128:(s + 1) * 128]

    def k_step(p):
        for e in range(2):
            q = 2 * p + e
            t = t_r[q]
            g = jnp.sum(t_f[q] * c_f[pl.ds(own_row, half), :] + t * c_f[pl.ds(oth_row, half), :])
            j_acc[...] += g * b_v[q]
            for k, part in enumerate(split3(t)):
                for s in range(2):
                    oth[k, s, :, e * 128:(e + 1) * 128] = part[:, s * 128:(s + 1) * 128]
        for s in range(2):
            wh, wm, wl = own[p, 0, s], own[p, 1, s], own[p, 2, s]
            oh, om, ol = oth[0, s], oth[1, s], oth[2, s]
            y_acc[s] += (mm_nt(wh * 0.5, wh) + mm_nt(wh, wm) + mm_nt(wm * 0.5, wm) + mm_nt(wh, wl))
            z_acc[s] += (mm_nt(oh, wh) + mm_nt(om, wh) + mm_nt(ol, wh) + mm_nt(oh, wm) + mm_nt(om, wm) + mm_nt(oh, wl))

    def first(p, carry):
        t_step(p)
        return carry

    def middle(p, carry):
        t_step(p)
        t_copy(p - 2).wait_recv()
        k_step(p - 2)
        t_copy(p).start()
        return carry

    def last(p, carry):
        t_copy(p).wait_recv()
        k_step(p)
        return carry

    t_step(0)
    pl.semaphore_wait(barrier, 10)
    t_copy(0).start()
    t_step(1)
    t_copy(1).start()
    lax.fori_loop(2, pairs, middle, 0)
    lax.fori_loop(pairs - 2, pairs, last, 0)
    lax.fori_loop(0, pairs, lambda p, carry: (t_copy(p).wait_send(), carry)[1], 0)

    j_own = j_acc[:, pl.ds(own_row, half)]
    j_oth = j_acc[:, pl.ds(oth_row, half)].T
    for s in range(2):
        y = y_acc[s]
        blocks = ((orb, j_own - (y + y.T)), (1 - orb, j_oth - z_acc[s]))
        for h in range(2):
            for where, block in blocks:
                p_buf[2 * s + h, pl.ds(2 * where, 2)] = block[:, h * 128:(h + 1) * 128].reshape(2, 4, 4, 8, 128)

    def ph_copy(phase, unit, dist):
        order = ORDERS[unit]
        device, target = peer(order[phase], dist)
        if phase == 0:
            axes, src, dst = [0, 1, 2], p_buf, r1
        elif phase == 1:
            axes, src, dst = sorted(order[1:]), s1, r2
        else:
            axes, src, dst = [order[2]], s2, r3
        where = tuple(target if a == order[phase] else slice(None) for a in axes)
        return pltpu.make_async_remote_copy(
            src_ref=src.at[(unit,) + where], dst_ref=dst.at[unit, dist - 1],
            send_sem=ph_send.at[phase, unit, dist - 1], recv_sem=ph_recv.at[phase, unit, dist - 1],
            device_id=device, device_id_type=MESH)

    def kept(phase, unit):
        order = ORDERS[unit]
        if phase == 0:
            axes, src = [0, 1, 2], p_buf
        elif phase == 1:
            axes, src = sorted(order[1:]), s1
        else:
            axes, src = [order[2]], s2
        where = tuple(coords[a] if a == order[phase] else slice(None) for a in axes)
        return src[(unit,) + where]

    for unit in range(4):
        for dist in (2, 1, 3):
            ph_copy(0, unit, dist).start()
    for phase in range(3):
        recv = (r1, r2, r3)[phase]
        for unit in range(4):
            for dist in (1, 2, 3):
                ph_copy(phase, unit, dist).wait_recv()
            total = kept(phase, unit) + recv[unit, 0] + recv[unit, 1] + recv[unit, 2]
            if phase < 2:
                (s1, s2)[phase][unit] = total
                for dist in (2, 1, 3):
                    ph_copy(phase + 1, unit, dist).start()
            else:
                s, h = divmod(unit, 2)
                o_ref[s, :, h * 128:(h + 1) * 128] = total
    for phase in range(3):
        for unit in range(4):
            for dist in (1, 2, 3):
                ph_copy(phase, unit, dist).wait_send()


def solution(mesh):
    def local_build(b_local, c_alpha, c_beta):
        n_q, half, rows = b_local.shape
        pairs = n_q // 2
        vmem = pltpu.VMEM
        dma = pltpu.SemaphoreType.DMA
        out = pl.pallas_call(
            functools.partial(kernel, n_q, rows),
            out_shape=jax.ShapeDtypeStruct((2, 8, half), F32),
            in_specs=[pl.BlockSpec(memory_space=pl.ANY), pl.BlockSpec(memory_space=vmem), pl.BlockSpec(memory_space=vmem)],
            out_specs=pl.BlockSpec(memory_space=vmem),
            scratch_shapes=[
                vmem((n_q, half, rows), F32),
                vmem((rows, 256), F32),
                vmem((3, rows, 256), BF16),
                vmem((n_q, half, 256), F32),
                vmem((n_q, half, 256), F32),
                vmem((pairs, 3, 2, half, 256), BF16),
                vmem((3, 2, half, 256), BF16),
                vmem((half, rows), F32),
                vmem((2, half, half), F32),
                vmem((2, half, half), F32),
                vmem((4, 4, 4, 4, 8, 128), F32),
                vmem((4, 3, 4, 4, 8, 128), F32),
                vmem((4, 4, 4, 8, 128), F32),
                vmem((4, 3, 4, 8, 128), F32),
                vmem((4, 4, 8, 128), F32),
                vmem((4, 3, 8, 128), F32),
                dma((n_q,)),
                dma((pairs,)),
                dma((pairs,)),
                dma((3, 4, 3)),
                dma((3, 4, 3)),
            ],
            compiler_params=pltpu.CompilerParams(
                collective_id=0, has_side_effects=True, vmem_limit_bytes=60 * 1024 * 1024),
        )(b_local, c_alpha, c_beta)
        return out[0].T, out[1].T

    spec_b = P(("sys", "aux"), "orb", None)
    spec_c = P("sys", None)
    spec_g = P(("sys", "orb"), "aux")
    return jax.shard_map(local_build, mesh=mesh, in_specs=(spec_b, spec_c, spec_c), out_specs=(spec_g, spec_g), check_vma=False)
```

```python
import functools

import jax
import jax.numpy as jnp
from jax import lax
from jax.experimental import pallas as pl
from jax.experimental.pallas import tpu as pltpu
from jax.sharding import PartitionSpec as P

MESH = pl.DeviceIdType.MESH
F32 = jnp.float32
BF16 = jnp.bfloat16
NT = (((1,), (1,)), ((), ()))
ORDERS = ((2, 1, 0), (1, 2, 0))
T_BLOCK = 2
K_BLOCK = 5


def split3(value):
    high = value.astype(BF16)
    rest = value - high.astype(F32)
    mid = rest.astype(BF16)
    low = (rest - mid.astype(F32)).astype(BF16)
    return high, mid, low


def mm(a, b):
    return jnp.dot(a, b, preferred_element_type=F32)


def mm_nt(a, b):
    return lax.dot_general(a, b, NT, preferred_element_type=F32)


def kernel(n_q, rows, b_ref, ca_ref, cb_ref, o_ref, b_v, ca_v, cb_v, c_pad, c_f, c_s, t_f, t_r, own, oth, j_acc, j_t, y_acc, z_acc,
           p_buf, r1, s1, r2, s2, r3, b_sem, c_sem, t_send, t_recv, send1, recv1, send2, recv2, send3, recv3):
    pairs = n_q // 2
    half = rows // 2
    aux = lax.axis_index("aux")
    orb = lax.axis_index("orb")
    coords = (aux // 16, lax.rem(aux // 4, 4), lax.rem(aux, 4))
    strides = (16, 4, 1)
    partner = {"aux": aux, "orb": 1 - orb}

    def peer(axis, dist):
        target = lax.rem(coords[axis] + dist, 4)
        return {"aux": aux + (target - coords[axis]) * strides[axis], "orb": orb}, target

    def b_copy(p):
        block = pl.ds(2 * p, 2)
        return pltpu.make_async_copy(b_ref.at[block], b_v.at[block], b_sem.at[p])

    c_copies = (pltpu.make_async_copy(ca_ref, ca_v, c_sem.at[0]), pltpu.make_async_copy(cb_ref, cb_v, c_sem.at[1]))
    for copy in c_copies:
        copy.start()
    for p in range(2 * T_BLOCK):
        b_copy(p).start()

    barrier = pltpu.get_barrier_semaphore()
    pl.semaphore_signal(barrier, inc=1, device_id=partner, device_id_type=MESH)
    for axis in range(3):
        for dist in (1, 2, 3):
            pl.semaphore_signal(barrier, inc=1, device_id=peer(axis, dist)[0], device_id_type=MESH)

    c_pad[...] = jnp.zeros_like(c_pad)
    for copy in c_copies:
        copy.wait()
    c_pad[0:ca_v.shape[0], :] = ca_v[...]
    c_pad[128:128 + cb_v.shape[0], :] = cb_v[...]
    c_all = c_pad[...].T
    c_f[...] = c_all
    for k, part in enumerate(split3(c_all)):
        c_s[k] = part
    own_row = pl.multiple_of(orb * half, half)
    oth_row = pl.multiple_of((1 - orb) * half, half)

    def t_copy(p):
        block = pl.ds(2 * p, 2)
        return pltpu.make_async_remote_copy(
            src_ref=t_f.at[block], dst_ref=t_r.at[block], send_sem=t_send.at[p], recv_sem=t_recv.at[p],
            device_id=partner, device_id_type=MESH)

    def t_step(p):
        for e in range(2):
            q = 2 * p + e
            h, m, l = split3(b_v[q])
            t = (mm(h, c_s[0]) + mm(m, c_s[0]) + mm(l, c_s[0]) + mm(h, c_s[1]) + mm(m, c_s[1]) + mm(h, c_s[2]))
            t_f[q] = t
            for k, part in enumerate(split3(t)):
                for s in range(2):
                    own[p, k, s, :, e * 128:(e + 1) * 128] = part[:, s * 128:(s + 1) * 128]

    def t_block(i, carry):
        for j in range(T_BLOCK):
            b_copy(T_BLOCK * i + j).wait()

        @pl.when(i < pairs // T_BLOCK - 2)
        def _():
            for j in range(T_BLOCK):
                b_copy(T_BLOCK * (i + 2) + j).start()

        for j in range(T_BLOCK):
            t_step(T_BLOCK * i + j)

        @pl.when(i == 0)
        def _():
            pl.semaphore_wait(barrier, 10)

        for j in range(T_BLOCK):
            t_copy(T_BLOCK * i + j).start()
        return carry

    lax.fori_loop(0, pairs // T_BLOCK, t_block, 0)

    def take(p, j, s):
        for e in range(2):
            for k, part in enumerate(split3(t_r[2 * p + e, :, s * 128:(s + 1) * 128])):
                oth[j, k, :, e * 128:(e + 1) * 128] = part

    def coulomb(p):
        total = None
        for e in range(2):
            q = 2 * p + e
            g = jnp.sum(t_f[q] * c_f[pl.ds(own_row, half), :] + t_r[q] * c_f[pl.ds(oth_row, half), :])
            term = g * b_v[q]
            total = term if total is None else total + term
        return total

    def own_terms(p, s):
        wh, wm, wl = own[p, 0, s], own[p, 1, s], own[p, 2, s]
        return mm_nt(wh * 0.5, wh) + mm_nt(wh, wm) + mm_nt(wm * 0.5, wm) + mm_nt(wh, wl)

    def oth_terms(p, j, s):
        wh, wm, wl = own[p, 0, s], own[p, 1, s], own[p, 2, s]
        oh, om, ol = oth[j, 0], oth[j, 1], oth[j, 2]
        return mm_nt(oh, wh) + mm_nt(om, wh) + mm_nt(ol, wh) + mm_nt(oh, wm) + mm_nt(om, wm) + mm_nt(oh, wl)

    def add(acc, i, value):
        acc[...] = value + jnp.where(i > 0, acc[...], 0.0)

    def alpha_block(i, carry):
        for j in range(K_BLOCK):
            t_copy(K_BLOCK * i + j).wait_recv()
        for j in range(K_BLOCK):
            take(K_BLOCK * i + j, j, 0)
        add(j_acc, i, sum(coulomb(K_BLOCK * i + j) for j in range(K_BLOCK)))
        add(y_acc, i, sum(own_terms(K_BLOCK * i + j, 0) for j in range(K_BLOCK)))
        add(z_acc, i, sum(oth_terms(K_BLOCK * i + j, j, 0) for j in range(K_BLOCK)))
        return carry

    def beta_oth_block(i, carry):
        for j in range(K_BLOCK):
            take(K_BLOCK * i + j, j, 1)
        add(z_acc, i, sum(oth_terms(K_BLOCK * i + j, j, 1) for j in range(K_BLOCK)))
        return carry

    def beta_own_block(i, carry):
        add(y_acc, i, sum(own_terms(K_BLOCK * i + j, 1) for j in range(K_BLOCK)))
        return carry

    z_pair = (pl.ds(2 * orb, 2), pl.ds(2 * (1 - orb), 2))

    def put(s, part, block):
        for h in range(2):
            p_buf[s, h, z_pair[part]] = block[:, h * 128:(h + 1) * 128].reshape(2, 4, 4, 8, 128)

    def at1(h, where):
        return (slice(None), where) if ORDERS[h][0] == 2 else (where,)

    def copy1(s, h, part, dist):
        device, target = peer(ORDERS[h][0], dist)
        return pltpu.make_async_remote_copy(
            src_ref=p_buf.at[(s, h, z_pair[part]) + at1(h, target)], dst_ref=r1.at[s, h, dist - 1, z_pair[part]],
            send_sem=send1.at[s, h, part, dist - 1], recv_sem=recv1.at[s, h, part, dist - 1],
            device_id=device, device_id_type=MESH)

    def copy2(s, h, dist):
        device, target = peer(ORDERS[h][1], dist)
        return pltpu.make_async_remote_copy(
            src_ref=s1.at[s, h, :, target], dst_ref=r2.at[s, h, dist - 1],
            send_sem=send2.at[s, h, dist - 1], recv_sem=recv2.at[s, h, dist - 1],
            device_id=device, device_id_type=MESH)

    def copy3(s, h, dist):
        device, target = peer(ORDERS[h][2], dist)
        return pltpu.make_async_remote_copy(
            src_ref=s2.at[s, h, target], dst_ref=r3.at[s, h, dist - 1],
            send_sem=send3.at[s, h, dist - 1], recv_sem=recv3.at[s, h, dist - 1],
            device_id=device, device_id_type=MESH)

    dists = (2, 1, 3)

    def start1(s, part):
        for dist in dists:
            for h in range(2):
                copy1(s, h, part, dist).start()

    def finish1(s):
        for part in (1, 0):
            for h in range(2):
                for dist in dists:
                    copy1(s, h, part, dist).wait_recv()
                zs = z_pair[part]
                s1[s, h, zs] = (p_buf[(s, h, zs) + at1(h, coords[ORDERS[h][0]])]
                                + r1[s, h, 0, zs] + r1[s, h, 1, zs] + r1[s, h, 2, zs])
        for dist in dists:
            for h in range(2):
                copy2(s, h, dist).start()

    def finish2(s):
        for h in range(2):
            for dist in dists:
                copy2(s, h, dist).wait_recv()
            s2[s, h] = s1[s, h, :, coords[ORDERS[h][1]]] + r2[s, h, 0] + r2[s, h, 1] + r2[s, h, 2]
        for dist in dists:
            for h in range(2):
                copy3(s, h, dist).start()

    def finish3(s):
        for h in range(2):
            for dist in dists:
                copy3(s, h, dist).wait_recv()
            o_ref[s, :, h * 128:(h + 1) * 128] = s2[s, h, coords[0]] + r3[s, h, 0] + r3[s, h, 1] + r3[s, h, 2]

    blocks = pairs // K_BLOCK
    lax.fori_loop(0, blocks, alpha_block, 0)
    j_t[...] = j_acc[:, pl.ds(oth_row, half)].T
    put(0, 1, j_t[...] - z_acc[...])
    put(0, 0, j_acc[:, pl.ds(own_row, half)] - (y_acc[...] + y_acc[...].T))
    start1(0, 1)
    start1(0, 0)
    lax.fori_loop(0, blocks, beta_oth_block, 0)
    put(1, 1, j_t[...] - z_acc[...])
    start1(1, 1)
    lax.fori_loop(0, blocks, beta_own_block, 0)
    put(1, 0, j_acc[:, pl.ds(own_row, half)] - (y_acc[...] + y_acc[...].T))
    start1(1, 0)
    finish1(0)
    finish1(1)
    finish2(0)
    finish2(1)
    finish3(0)
    finish3(1)
    lax.fori_loop(0, pairs, lambda p, carry: (t_copy(p).wait_send(), carry)[1], 0)
    for s in range(2):
        for h in range(2):
            for dist in dists:
                copy1(s, h, 0, dist).wait_send()
                copy1(s, h, 1, dist).wait_send()
                copy2(s, h, dist).wait_send()
                copy3(s, h, dist).wait_send()


def solution(mesh):
    def local_build(b_local, c_alpha, c_beta):
        n_q, half, rows = b_local.shape
        pairs = n_q // 2
        vmem = pltpu.VMEM
        dma = pltpu.SemaphoreType.DMA
        anywhere = pl.BlockSpec(memory_space=pl.ANY)
        out = pl.pallas_call(
            functools.partial(kernel, n_q, rows),
            out_shape=jax.ShapeDtypeStruct((2, 8, half), F32),
            in_specs=[anywhere, anywhere, anywhere],
            out_specs=pl.BlockSpec(memory_space=vmem),
            scratch_shapes=[
                vmem((n_q, half, rows), F32),
                vmem((c_alpha.shape[1], rows), F32),
                vmem((c_beta.shape[1], rows), F32),
                vmem((256, rows), F32),
                vmem((rows, 256), F32),
                vmem((3, rows, 256), BF16),
                vmem((n_q, half, 256), F32),
                vmem((n_q, half, 256), F32),
                vmem((pairs, 3, 2, half, 256), BF16),
                vmem((K_BLOCK, 3, half, 256), BF16),
                vmem((half, rows), F32),
                vmem((half, half), F32),
                vmem((half, half), F32),
                vmem((half, half), F32),
                vmem((2, 2, 4, 4, 4, 8, 128), F32),
                vmem((2, 2, 3, 4, 4, 8, 128), F32),
                vmem((2, 2, 4, 4, 8, 128), F32),
                vmem((2, 2, 3, 4, 8, 128), F32),
                vmem((2, 2, 4, 8, 128), F32),
                vmem((2, 2, 3, 8, 128), F32),
                dma((pairs,)),
                dma((2,)),
                dma((pairs,)),
                dma((pairs,)),
                dma((2, 2, 2, 3)),
                dma((2, 2, 2, 3)),
                dma((2, 2, 3)),
                dma((2, 2, 3)),
                dma((2, 2, 3)),
                dma((2, 2, 3)),
            ],
            compiler_params=pltpu.CompilerParams(
                collective_id=0, has_side_effects=True, vmem_limit_bytes=60 * 1024 * 1024),
        )(b_local, c_alpha.T, c_beta.T)
        return out[0].T, out[1].T

    spec_b = P(("sys", "aux"), "orb", None)
    spec_c = P("sys", None)
    spec_g = P(("sys", "orb"), "aux")
    return jax.shard_map(local_build, mesh=mesh, in_specs=(spec_b, spec_c, spec_c), out_specs=(spec_g, spec_g), check_vma=False)
```

```python
import functools

import jax
import jax.numpy as jnp
from jax import lax
from jax.experimental import pallas as pl
from jax.experimental.pallas import tpu as pltpu
from jax.sharding import PartitionSpec as P

MESH = pl.DeviceIdType.MESH
F32 = jnp.float32
BF16 = jnp.bfloat16
NT = (((1,), (1,)), ((), ()))
T_BLOCK = 5
X_FIRST, Y_FIRST, Z_FIRST = (2, 0, 1), (1, 0, 2), (0, 1, 2)
ORDERS = (((X_FIRST, Y_FIRST), (Y_FIRST, X_FIRST)), ((Z_FIRST, X_FIRST), (Y_FIRST, Z_FIRST)))


def split3(value):
    high = value.astype(BF16)
    rest = value - high.astype(F32)
    mid = rest.astype(BF16)
    low = (rest - mid.astype(F32)).astype(BF16)
    return high, mid, low


def mm(a, b):
    return jnp.dot(a, b, preferred_element_type=F32)


def mm_nt(a, b):
    return lax.dot_general(a, b, NT, preferred_element_type=F32)


def joined(ref):
    return jnp.concatenate([ref[i] for i in range(ref.shape[0])], axis=1)


def kernel(n_q, rows, *refs):
    (b_ref, ca_ref, cb_ref, o_ref, b_v, ca_v, cb_v, c_pad, c_f, c_s, t_f, t_r, g_f, g_r, own, oth, j_acc, j_t, y_acc, z_f, z_r,
     p_buf, r1, s1, r2, s2, r3, b_sem, c_sem, t_send, t_recv, g_send, g_recv, z_send, z_recv,
     send1, recv1, send2, recv2, send3, recv3) = refs
    pairs = n_q // 2
    shared = pairs // 2
    half = rows // 2
    aux = lax.axis_index("aux")
    orb = lax.axis_index("orb")
    coords = (aux // 16, lax.rem(aux // 4, 4), lax.rem(aux, 4))
    strides = (16, 4, 1)
    partner = {"aux": aux, "orb": 1 - orb}

    def peer(axis, dist):
        target = lax.rem(coords[axis] + dist, 4)
        return {"aux": aux + (target - coords[axis]) * strides[axis], "orb": orb}, target

    def b_copy(p):
        first = shared * (1 - orb)
        where = lax.rem(p + first, pairs)
        return pltpu.make_async_copy(b_ref.at[pl.ds(2 * where, 2)], b_v.at[pl.ds(2 * p, 2)], b_sem.at[p])

    c_copies = (pltpu.make_async_copy(ca_ref, ca_v, c_sem.at[0]), pltpu.make_async_copy(cb_ref, cb_v, c_sem.at[1]))
    for copy in c_copies:
        copy.start()
    for p in range(T_BLOCK):
        b_copy(p).start()

    barrier = pltpu.get_barrier_semaphore()
    pl.semaphore_signal(barrier, inc=1, device_id=partner, device_id_type=MESH)
    for axis in range(3):
        for dist in (1, 2, 3):
            pl.semaphore_signal(barrier, inc=1, device_id=peer(axis, dist)[0], device_id_type=MESH)

    c_pad[...] = jnp.zeros_like(c_pad)
    for copy in c_copies:
        copy.wait()
    c_pad[0:ca_v.shape[0], :] = ca_v[...]
    c_pad[128:128 + cb_v.shape[0], :] = cb_v[...]
    c_all = c_pad[...].T
    c_f[...] = c_all
    for k, part in enumerate(split3(c_all)):
        c_s[k, 0] = part[:, 0:128]
        c_s[k, 1] = part[:, 128:256]
    own_row = pl.multiple_of(orb * half, half)
    oth_row = pl.multiple_of((1 - orb) * half, half)

    def t_copy(p):
        return pltpu.make_async_remote_copy(
            src_ref=t_f.at[p], dst_ref=t_r.at[p], send_sem=t_send.at[p], recv_sem=t_recv.at[p],
            device_id=partner, device_id_type=MESH)

    def g_copy(p):
        there = lax.rem(p + shared, pairs)
        return pltpu.make_async_remote_copy(
            src_ref=g_f.at[p], dst_ref=g_r.at[there], send_sem=g_send.at[p], recv_sem=g_recv.at[there],
            device_id=partner, device_id_type=MESH)

    def g_landed(p):
        g_copy(lax.rem(p + shared, pairs)).wait_recv()

    def z_copy(s):
        return pltpu.make_async_remote_copy(
            src_ref=z_f.at[s], dst_ref=z_r.at[s], send_sem=z_send.at[s], recv_sem=z_recv.at[s],
            device_id=partner, device_id_type=MESH)

    def t_step(p):
        for e in range(2):
            h, m, l = split3(b_v[2 * p + e])
            ch, cm, cl = joined(c_s.at[0]), joined(c_s.at[1]), joined(c_s.at[2])
            t = mm(h, ch) + mm(m, ch) + mm(l, ch) + mm(h, cm) + mm(m, cm) + mm(h, cl)
            t_f[p, e] = t
            prod = (t * c_f[pl.ds(own_row, half), :]).reshape(half // 8, 8, 256).sum(axis=0)
            g_f[p, e] = prod[:, 0:128] + prod[:, 128:256]
            for k, part in enumerate(split3(t)):
                for s in range(2):
                    own[p, k, s, e] = part[:, s * 128:(s + 1) * 128]

    def send_t(p):
        g_copy(p).start()

        @pl.when(p < shared)
        def _():
            t_copy(p).start()

    def t_block(i, carry):
        p = T_BLOCK * i

        @pl.when(i == 0)
        def _():
            for j in range(T_BLOCK, pairs):
                b_copy(j).start()

        for j in range(T_BLOCK):
            b_copy(p + j).wait()
            t_step(p + j)

        @pl.when(i == 0)
        def _():
            pl.semaphore_wait(barrier, 10)

        for j in range(T_BLOCK):
            send_t(p + j)
        return carry

    lax.fori_loop(0, pairs // T_BLOCK, t_block, 0)

    def take(s):
        for j in range(shared):
            for e in range(2):
                for k, part in enumerate(split3(t_r[j, e, :, s * 128:(s + 1) * 128])):
                    oth[s, j, k, e] = part

    def coulomb():
        g = [jnp.sum(g_f[q // 2, q % 2] + g_r[q // 2, q % 2]) for q in range(n_q)]
        for row in range(0, half, 8):
            total = g[0] * b_v[0, row:row + 8, :]
            for q in range(1, n_q):
                total = total + g[q] * b_v[q, row:row + 8, :]
            j_acc[row:row + 8, :] = total

    def own_sum(s, ps):
        total = None
        for p in ps:
            wh, wm, wl = (joined(own.at[p, k, s]) for k in range(3))
            term = mm_nt(wh * 0.5, wh) + mm_nt(wm, wh) + mm_nt(wl, wh) + mm_nt(wm * 0.5, wm)
            total = term if total is None else total + term
        return total

    def oth_sum(s, work):
        total = None
        for j, parts in work:
            for k in parts:
                right = joined(own.at[shared + j, k, s])
                for lhs in range(3 - k):
                    term = mm_nt(joined(oth.at[s, j, lhs]), right)
                    total = term if total is None else total + term
        return total

    def own_products(s):
        return own_sum(s, range(pairs))

    def oth_products(s):
        return oth_sum(s, [(j, (0, 1, 2)) for j in range(shared)])

    def block(body):
        def trip(_, carry):
            body()
            return carry
        lax.fori_loop(orb, orb + 1, trip, 0)

    z_pair = (pl.ds(2 * orb, 2), pl.ds(2 * (1 - orb), 2))

    def put(s, part, block):
        for h in range(2):
            p_buf[s, h, z_pair[part]] = block[:, h * 128:(h + 1) * 128].reshape(2, 4, 4, 8, 128)

    def put_own(s):
        put(s, 0, j_acc[:, pl.ds(own_row, half)] - (y_acc[...] + y_acc[...].T))

    def put_oth(s):
        put(s, 1, j_t[...] - z_f[s] - z_r[s].T)

    def by_core(body, *args):
        for r in range(2):
            @pl.when(orb == r)
            def _():
                body(r, *args)

    dists = (2, 1, 3)

    def line1(axis, zs, where):
        return {0: (where,), 1: (zs, where), 2: (zs, slice(None), where)}[axis]

    def copy1(r, s, h, part, dist):
        axis = ORDERS[r][s][h][0]
        zs = pl.ds(2 * (r if part == 0 else 1 - r), 2)
        device, target = peer(axis, dist)
        dst = r1.at[s, h, dist - 1] if axis == 0 else r1.at[s, h, dist - 1, zs]
        return pltpu.make_async_remote_copy(
            src_ref=p_buf.at[(s, h) + line1(axis, zs, target)], dst_ref=dst,
            send_sem=send1.at[s, h, part, dist - 1], recv_sem=recv1.at[s, h, part, dist - 1],
            device_id=device, device_id_type=MESH)

    def copy2(r, s, h, dist):
        order = ORDERS[r][s][h]
        device, target = peer(order[1], dist)
        where = (target,) if order[1] == min(order[1:]) else (slice(None), target)
        return pltpu.make_async_remote_copy(
            src_ref=s1.at[(s, h) + where], dst_ref=r2.at[s, h, dist - 1],
            send_sem=send2.at[s, h, dist - 1], recv_sem=recv2.at[s, h, dist - 1],
            device_id=device, device_id_type=MESH)

    def copy3(r, s, h, dist):
        device, target = peer(ORDERS[r][s][h][2], dist)
        return pltpu.make_async_remote_copy(
            src_ref=s2.at[s, h, target], dst_ref=r3.at[s, h, dist - 1],
            send_sem=send3.at[s, h, dist - 1], recv_sem=recv3.at[s, h, dist - 1],
            device_id=device, device_id_type=MESH)

    def start1(r, s, part):
        for dist in dists:
            for h in range(2):
                if ORDERS[r][s][h][0] == 0:
                    @pl.when((peer(0, dist)[1] // 2 == r) == (part == 0))
                    def _():
                        copy1(r, s, h, 0, dist).start()
                else:
                    copy1(r, s, h, part, dist).start()

    def parts1(r, s, h):
        return (0,) if ORDERS[r][s][h][0] == 0 else (1, 0)

    def finish1(r, s):
        for h in range(2):
            axis = ORDERS[r][s][h][0]
            for part in parts1(r, s, h):
                for dist in dists:
                    copy1(r, s, h, part, dist).wait_recv()
                zs = pl.ds(2 * (r if part == 0 else 1 - r), 2)
                kept = p_buf[(s, h) + line1(axis, zs, coords[axis])]
                if axis == 0:
                    s1[s, h] = kept + r1[s, h, 0] + r1[s, h, 1] + r1[s, h, 2]
                else:
                    s1[s, h, zs] = kept + r1[s, h, 0, zs] + r1[s, h, 1, zs] + r1[s, h, 2, zs]
            for dist in dists:
                copy2(r, s, h, dist).start()

    def finish2(r, s):
        for h in range(2):
            order = ORDERS[r][s][h]
            for dist in dists:
                copy2(r, s, h, dist).wait_recv()
            where = (coords[order[1]],) if order[1] == min(order[1:]) else (slice(None), coords[order[1]])
            s2[s, h] = s1[(s, h) + where] + r2[s, h, 0] + r2[s, h, 1] + r2[s, h, 2]
            for dist in dists:
                copy3(r, s, h, dist).start()

    def finish3(r, s):
        for h in range(2):
            for dist in dists:
                copy3(r, s, h, dist).wait_recv()
            o_ref[s, :, h * 128:(h + 1) * 128] = (
                s2[s, h, coords[ORDERS[r][s][h][2]]] + r3[s, h, 0] + r3[s, h, 1] + r3[s, h, 2])

    def sent(r):
        for s in range(2):
            for h in range(2):
                for dist in dists:
                    for part in parts1(r, s, h):
                        copy1(r, s, h, part, dist).wait_send()
                    copy2(r, s, h, dist).wait_send()
                    copy3(r, s, h, dist).wait_send()

    def reduce_rest(r):
        for s in range(2):
            finish1(r, s)
        for s in range(2):
            finish2(r, s)
        for s in range(2):
            finish3(r, s)
        sent(r)

    def alpha_oth():
        take(0)
        z_f[0] = oth_products(0)
        take(1)

    def beta_oth():
        z_f[1] = oth_products(1)
        coulomb()

    def alpha_own():
        y_acc[...] = own_products(0)

    def beta_own():
        y_acc[...] = own_products(1)

    for p in range(shared):
        t_copy(p).wait_recv()
    block(alpha_oth)
    z_copy(0).start()
    for p in range(pairs):
        g_landed(p)
    block(beta_oth)
    z_copy(1).start()
    z_copy(0).wait_recv()
    j_t[...] = j_acc[:, pl.ds(oth_row, half)].T
    put_oth(0)
    by_core(start1, 0, 1)
    block(alpha_own)
    put_own(0)
    by_core(start1, 0, 0)
    z_copy(1).wait_recv()
    put_oth(1)
    by_core(start1, 1, 1)
    block(beta_own)
    put_own(1)
    by_core(start1, 1, 0)
    by_core(reduce_rest)
    for p in range(shared):
        t_copy(p).wait_send()
    for p in range(pairs):
        g_copy(p).wait_send()
    for s in range(2):
        z_copy(s).wait_send()


def solution(mesh):
    def local_build(b_local, c_alpha, c_beta):
        n_q, half, rows = b_local.shape
        pairs = n_q // 2
        vmem = pltpu.VMEM
        dma = pltpu.SemaphoreType.DMA
        anywhere = pl.BlockSpec(memory_space=pl.ANY)
        out = pl.pallas_call(
            functools.partial(kernel, n_q, rows),
            out_shape=jax.ShapeDtypeStruct((2, 8, half), F32),
            in_specs=[anywhere, anywhere, anywhere],
            out_specs=pl.BlockSpec(memory_space=vmem),
            scratch_shapes=[
                vmem((n_q, half, rows), F32),
                vmem((c_alpha.shape[1], rows), F32),
                vmem((c_beta.shape[1], rows), F32),
                vmem((256, rows), F32),
                vmem((rows, 256), F32),
                vmem((3, 2, rows, 128), BF16),
                vmem((pairs, 2, half, 256), F32),
                vmem((pairs // 2, 2, half, 256), F32),
                vmem((pairs, 2, 8, 128), F32),
                vmem((pairs, 2, 8, 128), F32),
                vmem((pairs, 3, 2, 2, half, 128), BF16),
                vmem((2, pairs // 2, 3, 2, half, 128), BF16),
                vmem((half, rows), F32),
                vmem((half, half), F32),
                vmem((half, half), F32),
                vmem((2, half, half), F32),
                vmem((2, half, half), F32),
                vmem((2, 2, 4, 4, 4, 8, 128), F32),
                vmem((2, 2, 3, 4, 4, 8, 128), F32),
                vmem((2, 2, 4, 4, 8, 128), F32),
                vmem((2, 2, 3, 4, 8, 128), F32),
                vmem((2, 2, 4, 8, 128), F32),
                vmem((2, 2, 3, 8, 128), F32),
                dma((pairs,)),
                dma((2,)),
                dma((pairs // 2,)),
                dma((pairs // 2,)),
                dma((pairs,)),
                dma((pairs,)),
                dma((2,)),
                dma((2,)),
                dma((2, 2, 2, 3)),
                dma((2, 2, 2, 3)),
                dma((2, 2, 3)),
                dma((2, 2, 3)),
                dma((2, 2, 3)),
                dma((2, 2, 3)),
            ],
            compiler_params=pltpu.CompilerParams(
                collective_id=0, has_side_effects=True, vmem_limit_bytes=60 * 1024 * 1024),
        )(b_local, c_alpha.T, c_beta.T)
        return out[0].T, out[1].T

    spec_b = P(("sys", "aux"), "orb", None)
    spec_c = P("sys", None)
    spec_g = P(("sys", "orb"), "aux")
    return jax.shard_map(local_build, mesh=mesh, in_specs=(spec_b, spec_c, spec_c), out_specs=(spec_g, spec_g), check_vma=False)
```

```python
import functools

import jax
import jax.numpy as jnp
from jax import lax
from jax.experimental import pallas as pl
from jax.experimental.pallas import tpu as pltpu
from jax.sharding import PartitionSpec as P

MESH = pl.DeviceIdType.MESH
F32 = jnp.float32
BF16 = jnp.bfloat16
NT = (((1,), (1,)), ((), ()))
T_BLOCK = 5
X_FIRST, Y_FIRST, Z_FIRST = (2, 0, 1), (1, 0, 2), (0, 1, 2)
ORDERS = (((X_FIRST, Y_FIRST), (Y_FIRST, X_FIRST)), ((Z_FIRST, X_FIRST), (Y_FIRST, Z_FIRST)))


def split3(value):
    high = value.astype(BF16)
    rest = value - high.astype(F32)
    mid = rest.astype(BF16)
    low = (rest - mid.astype(F32)).astype(BF16)
    return high, mid, low


def mm(a, b):
    return jnp.dot(a, b, preferred_element_type=F32)


def mm_nt(a, b):
    return lax.dot_general(a, b, NT, preferred_element_type=F32)


def joined(ref):
    return jnp.concatenate([ref[i] for i in range(ref.shape[0])], axis=1)


def kernel(n_q, rows, *refs):
    (b_ref, ca_ref, cb_ref, o_ref, b_v, ca_v, cb_v, c_pad, c_f, c_s, t_f, t_r, g_f, g_r, own, oth, j_acc, j_t, y_acc, z_f, z_r,
     p_buf, r1, s1, r2, s2, r3, b_sem, c_sem, t_send, t_recv, g_send, g_recv, z_send, z_recv,
     send1, recv1, send2, recv2, send3, recv3) = refs
    pairs = n_q // 2
    shared = pairs // 2
    half = rows // 2
    aux = lax.axis_index("aux")
    orb = lax.axis_index("orb")
    coords = (aux // 16, lax.rem(aux // 4, 4), lax.rem(aux, 4))
    strides = (16, 4, 1)
    partner = {"aux": aux, "orb": 1 - orb}

    def peer(axis, dist):
        target = lax.rem(coords[axis] + dist, 4)
        return {"aux": aux + (target - coords[axis]) * strides[axis], "orb": orb}, target

    def b_copy(p):
        first = shared * (1 - orb)
        where = lax.rem(p + first, pairs)
        return pltpu.make_async_copy(b_ref.at[pl.ds(2 * where, 2)], b_v.at[pl.ds(2 * p, 2)], b_sem.at[p])

    c_copies = (pltpu.make_async_copy(ca_ref, ca_v, c_sem.at[0]), pltpu.make_async_copy(cb_ref, cb_v, c_sem.at[1]))
    for copy in c_copies:
        copy.start()
    for p in range(T_BLOCK):
        b_copy(p).start()

    barrier = pltpu.get_barrier_semaphore()
    pl.semaphore_signal(barrier, inc=1, device_id=partner, device_id_type=MESH)
    for axis in range(3):
        for dist in (1, 2, 3):
            pl.semaphore_signal(barrier, inc=1, device_id=peer(axis, dist)[0], device_id_type=MESH)

    c_pad[...] = jnp.zeros_like(c_pad)
    for copy in c_copies:
        copy.wait()
    c_pad[0:ca_v.shape[0], :] = ca_v[...]
    c_pad[128:128 + cb_v.shape[0], :] = cb_v[...]
    c_all = c_pad[...].T
    c_f[...] = c_all
    for k, part in enumerate(split3(c_all)):
        c_s[k, 0] = part[:, 0:128]
        c_s[k, 1] = part[:, 128:256]
    own_row = pl.multiple_of(orb * half, half)
    oth_row = pl.multiple_of((1 - orb) * half, half)

    def t_copy(p):
        return pltpu.make_async_remote_copy(
            src_ref=t_f.at[p], dst_ref=t_r.at[p], send_sem=t_send.at[p], recv_sem=t_recv.at[p],
            device_id=partner, device_id_type=MESH)

    def g_copy(p):
        there = lax.rem(p + shared, pairs)
        return pltpu.make_async_remote_copy(
            src_ref=g_f.at[p], dst_ref=g_r.at[there], send_sem=g_send.at[p], recv_sem=g_recv.at[there],
            device_id=partner, device_id_type=MESH)

    def g_landed(p):
        g_copy(lax.rem(p + shared, pairs)).wait_recv()

    def z_copy(s):
        return pltpu.make_async_remote_copy(
            src_ref=z_f.at[s], dst_ref=z_r.at[s], send_sem=z_send.at[s], recv_sem=z_recv.at[s],
            device_id=partner, device_id_type=MESH)

    def t_step(p):
        for e in range(2):
            h, m, l = split3(b_v[2 * p + e])
            ch, cm, cl = joined(c_s.at[0]), joined(c_s.at[1]), joined(c_s.at[2])
            t = mm(h, ch) + mm(m, ch) + mm(l, ch) + mm(h, cm) + mm(m, cm) + mm(h, cl)
            t_f[p, e] = t
            prod = (t * c_f[pl.ds(own_row, half), :]).reshape(half // 8, 8, 256).sum(axis=0)
            g_f[p, e] = prod[:, 0:128] + prod[:, 128:256]
            for k, part in enumerate(split3(t)):
                for s in range(2):
                    own[p, k, s, e] = part[:, s * 128:(s + 1) * 128]

    def send_t(p):
        g_copy(p).start()

        @pl.when(p < shared)
        def _():
            t_copy(p).start()

    def t_block(i, carry):
        p = T_BLOCK * i

        @pl.when(i == 0)
        def _():
            for j in range(T_BLOCK, pairs):
                b_copy(j).start()

        for j in range(T_BLOCK):
            b_copy(p + j).wait()
            t_step(p + j)

        @pl.when(i == 0)
        def _():
            pl.semaphore_wait(barrier, 10)

        for j in range(T_BLOCK):
            send_t(p + j)
        return carry

    lax.fori_loop(0, pairs // T_BLOCK, t_block, 0)

    def take(s):
        for j in range(shared):
            for e in range(2):
                for k, part in enumerate(split3(t_r[j, e, :, s * 128:(s + 1) * 128])):
                    oth[s, j, k, e] = part

    def coulomb():
        g = [jnp.sum(g_f[q // 2, q % 2] + g_r[q // 2, q % 2]) for q in range(n_q)]
        for row in range(0, half, 8):
            total = g[0] * b_v[0, row:row + 8, :]
            for q in range(1, n_q):
                total = total + g[q] * b_v[q, row:row + 8, :]
            j_acc[row:row + 8, :] = total

    def own_sum(s, ps):
        total = None
        for p in ps:
            wh, wm, wl = (joined(own.at[p, k, s]) for k in range(3))
            term = mm_nt(wh * 0.5, wh) + mm_nt(wm, wh) + mm_nt(wl, wh) + mm_nt(wm * 0.5, wm)
            total = term if total is None else total + term
        return total

    def oth_sum(s, work):
        total = None
        for j, parts in work:
            for k in parts:
                right = joined(own.at[shared + j, k, s])
                for lhs in range(3 - k):
                    term = mm_nt(joined(oth.at[s, j, lhs]), right)
                    total = term if total is None else total + term
        return total

    def own_products(s):
        return own_sum(s, range(pairs))

    def oth_products(s):
        return oth_sum(s, [(j, (0, 1, 2)) for j in range(shared)])

    def block(body):
        def trip(_, carry):
            body()
            return carry
        lax.fori_loop(orb, orb + 1, trip, 0)

    z_pair = (pl.ds(2 * orb, 2), pl.ds(2 * (1 - orb), 2))

    def put(s, part, block):
        for h in range(2):
            p_buf[s, h, z_pair[part]] = block[:, h * 128:(h + 1) * 128].reshape(2, 4, 4, 8, 128)

    def put_own(s):
        put(s, 0, j_acc[:, pl.ds(own_row, half)] - (y_acc[...] + y_acc[...].T))

    def put_oth(s):
        put(s, 1, j_t[...] - z_f[s] - z_r[s].T)

    def by_core(body, *args):
        for r in range(2):
            @pl.when(orb == r)
            def _():
                body(r, *args)

    dists = (2, 1, 3)

    def line1(axis, zs, where):
        return {0: (where,), 1: (zs, where), 2: (zs, slice(None), where)}[axis]

    def copy1(r, s, h, part, dist):
        axis = ORDERS[r][s][h][0]
        zs = pl.ds(2 * (r if part == 0 else 1 - r), 2)
        device, target = peer(axis, dist)
        dst = r1.at[s, h, dist - 1] if axis == 0 else r1.at[s, h, dist - 1, zs]
        return pltpu.make_async_remote_copy(
            src_ref=p_buf.at[(s, h) + line1(axis, zs, target)], dst_ref=dst,
            send_sem=send1.at[s, h, part, dist - 1], recv_sem=recv1.at[s, h, part, dist - 1],
            device_id=device, device_id_type=MESH)

    def copy2(r, s, h, dist):
        order = ORDERS[r][s][h]
        device, target = peer(order[1], dist)
        where = (target,) if order[1] == min(order[1:]) else (slice(None), target)
        return pltpu.make_async_remote_copy(
            src_ref=s1.at[(s, h) + where], dst_ref=r2.at[s, h, dist - 1],
            send_sem=send2.at[s, h, dist - 1], recv_sem=recv2.at[s, h, dist - 1],
            device_id=device, device_id_type=MESH)

    def copy3(r, s, h, dist):
        device, target = peer(ORDERS[r][s][h][2], dist)
        return pltpu.make_async_remote_copy(
            src_ref=s2.at[s, h, target], dst_ref=r3.at[s, h, dist - 1],
            send_sem=send3.at[s, h, dist - 1], recv_sem=recv3.at[s, h, dist - 1],
            device_id=device, device_id_type=MESH)

    def start1(r, s, part):
        for dist in dists:
            for h in range(2):
                if ORDERS[r][s][h][0] == 0:
                    @pl.when((peer(0, dist)[1] // 2 == r) == (part == 0))
                    def _():
                        copy1(r, s, h, 0, dist).start()
                else:
                    copy1(r, s, h, part, dist).start()

    def parts1(r, s, h):
        return (0,) if ORDERS[r][s][h][0] == 0 else (1, 0)

    def finish1(r, s):
        for h in range(2):
            axis = ORDERS[r][s][h][0]
            for part in parts1(r, s, h):
                for dist in dists:
                    copy1(r, s, h, part, dist).wait_recv()
                zs = pl.ds(2 * (r if part == 0 else 1 - r), 2)
                kept = p_buf[(s, h) + line1(axis, zs, coords[axis])]
                if axis == 0:
                    s1[s, h] = kept + r1[s, h, 0] + r1[s, h, 1] + r1[s, h, 2]
                else:
                    s1[s, h, zs] = kept + r1[s, h, 0, zs] + r1[s, h, 1, zs] + r1[s, h, 2, zs]
            for dist in dists:
                copy2(r, s, h, dist).start()

    def finish2(r, s):
        for h in range(2):
            order = ORDERS[r][s][h]
            for dist in dists:
                copy2(r, s, h, dist).wait_recv()
            where = (coords[order[1]],) if order[1] == min(order[1:]) else (slice(None), coords[order[1]])
            s2[s, h] = s1[(s, h) + where] + r2[s, h, 0] + r2[s, h, 1] + r2[s, h, 2]
            for dist in dists:
                copy3(r, s, h, dist).start()

    def finish3(r, s):
        for h in range(2):
            for dist in dists:
                copy3(r, s, h, dist).wait_recv()
            o_ref[s, :, h * 128:(h + 1) * 128] = (
                s2[s, h, coords[ORDERS[r][s][h][2]]] + r3[s, h, 0] + r3[s, h, 1] + r3[s, h, 2])

    def sent(r):
        for s in range(2):
            for h in range(2):
                for dist in dists:
                    for part in parts1(r, s, h):
                        copy1(r, s, h, part, dist).wait_send()
                    copy2(r, s, h, dist).wait_send()
                    copy3(r, s, h, dist).wait_send()

    def reduce_rest(r):
        for s in range(2):
            finish1(r, s)
        for s in range(2):
            finish2(r, s)
        for s in range(2):
            finish3(r, s)
        sent(r)

    def alpha_oth():
        take(0)
        z_f[0] = oth_products(0)
        take(1)

    def beta_oth():
        z_f[1] = oth_products(1)
        coulomb()

    def alpha_own():
        y_acc[...] = own_products(0)

    def beta_own():
        y_acc[...] = own_products(1)

    for p in range(shared):
        t_copy(p).wait_recv()
    block(alpha_oth)
    z_copy(0).start()
    for p in range(pairs):
        g_landed(p)
    block(beta_oth)
    z_copy(1).start()
    z_copy(0).wait_recv()
    j_t[...] = j_acc[:, pl.ds(oth_row, half)].T
    put_oth(0)
    by_core(start1, 0, 1)
    block(alpha_own)
    put_own(0)
    by_core(start1, 0, 0)
    z_copy(1).wait_recv()
    put_oth(1)
    by_core(start1, 1, 1)
    block(beta_own)
    put_own(1)
    by_core(start1, 1, 0)
    by_core(reduce_rest)
    for p in range(shared):
        t_copy(p).wait_send()
    for p in range(pairs):
        g_copy(p).wait_send()
    for s in range(2):
        z_copy(s).wait_send()


def solution(mesh):
    def local_build(b_local, c_alpha, c_beta):
        n_q, half, rows = b_local.shape
        pairs = n_q // 2
        vmem = pltpu.VMEM
        dma = pltpu.SemaphoreType.DMA
        anywhere = pl.BlockSpec(memory_space=pl.ANY)
        out = pl.pallas_call(
            functools.partial(kernel, n_q, rows),
            out_shape=pltpu.VMEM((2, 8, half), F32),
            in_specs=[anywhere, anywhere, anywhere],
            out_specs=pl.BlockSpec(memory_space=vmem),
            scratch_shapes=[
                vmem((n_q, half, rows), F32),
                vmem((c_alpha.shape[1], rows), F32),
                vmem((c_beta.shape[1], rows), F32),
                vmem((256, rows), F32),
                vmem((rows, 256), F32),
                vmem((3, 2, rows, 128), BF16),
                vmem((pairs, 2, half, 256), F32),
                vmem((pairs // 2, 2, half, 256), F32),
                vmem((pairs, 2, 8, 128), F32),
                vmem((pairs, 2, 8, 128), F32),
                vmem((pairs, 3, 2, 2, half, 128), BF16),
                vmem((2, pairs // 2, 3, 2, half, 128), BF16),
                vmem((half, rows), F32),
                vmem((half, half), F32),
                vmem((half, half), F32),
                vmem((2, half, half), F32),
                vmem((2, half, half), F32),
                vmem((2, 2, 4, 4, 4, 8, 128), F32),
                vmem((2, 2, 3, 4, 4, 8, 128), F32),
                vmem((2, 2, 4, 4, 8, 128), F32),
                vmem((2, 2, 3, 4, 8, 128), F32),
                vmem((2, 2, 4, 8, 128), F32),
                vmem((2, 2, 3, 8, 128), F32),
                dma((pairs,)),
                dma((2,)),
                dma((pairs // 2,)),
                dma((pairs // 2,)),
                dma((pairs,)),
                dma((pairs,)),
                dma((2,)),
                dma((2,)),
                dma((2, 2, 2, 3)),
                dma((2, 2, 2, 3)),
                dma((2, 2, 3)),
                dma((2, 2, 3)),
                dma((2, 2, 3)),
                dma((2, 2, 3)),
            ],
            compiler_params=pltpu.CompilerParams(
                collective_id=0, has_side_effects=True, vmem_limit_bytes=60 * 1024 * 1024),
        )(b_local, c_alpha.T, c_beta.T)
        return out[0].T, out[1].T

    spec_b = P(("sys", "aux"), "orb", None)
    spec_c = P("sys", None)
    spec_g = P(("sys", "orb"), "aux")
    return jax.shard_map(local_build, mesh=mesh, in_specs=(spec_b, spec_c, spec_c), out_specs=(spec_g, spec_g), check_vma=False)
```

```python
import functools

import jax
import jax.numpy as jnp
from jax import lax
from jax.experimental import pallas as pl
from jax.experimental.pallas import tpu as pltpu
from jax.sharding import PartitionSpec as P

MESH = pl.DeviceIdType.MESH
F32 = jnp.float32
BF16 = jnp.bfloat16
NT = (((1,), (1,)), ((), ()))
T_BLOCKS = (1, 4, 5)
X_FIRST, Y_FIRST, Z_FIRST = (2, 0, 1), (1, 0, 2), (0, 1, 2)
ORDERS = (((X_FIRST, Y_FIRST), (Y_FIRST, X_FIRST)), ((Z_FIRST, X_FIRST), (Y_FIRST, Z_FIRST)))


def split3(value):
    high = value.astype(BF16)
    rest = value - high.astype(F32)
    mid = rest.astype(BF16)
    low = (rest - mid.astype(F32)).astype(BF16)
    return high, mid, low


def mm(a, b):
    return jnp.dot(a, b, preferred_element_type=F32)


def mm_nt(a, b):
    return lax.dot_general(a, b, NT, preferred_element_type=F32)


def joined(ref):
    return jnp.concatenate([ref[i] for i in range(ref.shape[0])], axis=1)


def kernel(n_q, rows, *refs):
    (b_ref, ca_ref, cb_ref, o_ref, b_v, ca_v, cb_v, c_pad, c_f, c_s, t_f, t_r, g_f, g_r, own, oth, j_acc, j_t, y_acc, z_f, z_r,
     p_buf, r1, s1, r2, s2, r3, b_sem, c_sem, t_send, t_recv, g_send, g_recv, z_send, z_recv,
     send1, recv1, send2, recv2, send3, recv3) = refs
    pairs = n_q // 2
    shared = pairs // 2
    half = rows // 2
    aux = lax.axis_index("aux")
    orb = lax.axis_index("orb")
    coords = (aux // 16, lax.rem(aux // 4, 4), lax.rem(aux, 4))
    strides = (16, 4, 1)
    partner = {"aux": aux, "orb": 1 - orb}

    def peer(axis, dist):
        target = lax.rem(coords[axis] + dist, 4)
        return {"aux": aux + (target - coords[axis]) * strides[axis], "orb": orb}, target

    def b_copy(p):
        first = shared * (1 - orb)
        where = lax.rem(p + first, pairs)
        return pltpu.make_async_copy(b_ref.at[pl.ds(2 * where, 2)], b_v.at[pl.ds(2 * p, 2)], b_sem.at[p])

    c_copies = (pltpu.make_async_copy(ca_ref, ca_v, c_sem.at[0]), pltpu.make_async_copy(cb_ref, cb_v, c_sem.at[1]))
    for copy in c_copies:
        copy.start()
    for p in range(T_BLOCKS[0] + T_BLOCKS[1]):
        b_copy(p).start()

    barrier = pltpu.get_barrier_semaphore()
    pl.semaphore_signal(barrier, inc=1, device_id=partner, device_id_type=MESH)
    for axis in range(3):
        for dist in (1, 2, 3):
            pl.semaphore_signal(barrier, inc=1, device_id=peer(axis, dist)[0], device_id_type=MESH)

    c_pad[...] = jnp.zeros_like(c_pad)
    for copy in c_copies:
        copy.wait()
    c_pad[0:ca_v.shape[0], :] = ca_v[...]
    c_pad[128:128 + cb_v.shape[0], :] = cb_v[...]
    c_all = c_pad[...].T
    c_f[...] = c_all
    for k, part in enumerate(split3(c_all)):
        c_s[k, 0] = part[:, 0:128]
        c_s[k, 1] = part[:, 128:256]
    own_row = pl.multiple_of(orb * half, half)
    oth_row = pl.multiple_of((1 - orb) * half, half)

    def t_copy(p):
        return pltpu.make_async_remote_copy(
            src_ref=t_f.at[p], dst_ref=t_r.at[p], send_sem=t_send.at[p], recv_sem=t_recv.at[p],
            device_id=partner, device_id_type=MESH)

    def g_copy(p):
        there = lax.rem(p + shared, pairs)
        return pltpu.make_async_remote_copy(
            src_ref=g_f.at[p], dst_ref=g_r.at[there], send_sem=g_send.at[p], recv_sem=g_recv.at[there],
            device_id=partner, device_id_type=MESH)

    def g_landed(p):
        g_copy(lax.rem(p + shared, pairs)).wait_recv()

    def z_copy(s):
        return pltpu.make_async_remote_copy(
            src_ref=z_f.at[s], dst_ref=z_r.at[s], send_sem=z_send.at[s], recv_sem=z_recv.at[s],
            device_id=partner, device_id_type=MESH)

    def t_step(p):
        for e in range(2):
            h, m, l = split3(b_v[2 * p + e])
            ch, cm, cl = joined(c_s.at[0]), joined(c_s.at[1]), joined(c_s.at[2])
            t = mm(h, ch) + mm(m, ch) + mm(l, ch) + mm(h, cm) + mm(m, cm) + mm(h, cl)
            t_f[p, e] = t
            prod = (t * c_f[pl.ds(own_row, half), :]).reshape(half // 8, 8, 256).sum(axis=0)
            g_f[p, e] = prod[:, 0:128] + prod[:, 128:256]
            for k, part in enumerate(split3(t)):
                for s in range(2):
                    own[p, k, s, e] = part[:, s * 128:(s + 1) * 128]

    def send_t(p):
        g_copy(p).start()

        if p < shared:
            t_copy(p).start()

    start = 0
    for i, size in enumerate(T_BLOCKS):
        ps = range(start, start + size)
        start += size
        for p in ps:
            b_copy(p).wait()
        if i == 0:
            for p in range(T_BLOCKS[0] + T_BLOCKS[1], pairs):
                b_copy(p).start()
        for p in ps:
            t_step(p)
        if i == 0:
            pl.semaphore_wait(barrier, 10)
        for p in ps:
            send_t(p)

    def take(s):
        for j in range(shared):
            for e in range(2):
                for k, part in enumerate(split3(t_r[j, e, :, s * 128:(s + 1) * 128])):
                    oth[s, j, k, e] = part

    def coulomb(ps, cols, width, old=None):
        qs = [(p, e) for p in ps for e in range(2)]
        g = [jnp.sum(g_f[q] + g_r[q]) for q in qs]
        out = []
        for row in range(0, half, 8):
            total = None if old is None else old[row:row + 8, :]
            for gq, (p, e) in zip(g, qs):
                term = gq * b_v[2 * p + e, row:row + 8, pl.ds(cols, width)]
                total = term if total is None else total + term
            out.append(total)
        return jnp.concatenate(out, axis=0)

    def own_sum(s, ps):
        total = None
        for p in ps:
            wh, wm, wl = (joined(own.at[p, k, s]) for k in range(3))
            term = mm_nt(wh * 0.5, wh) + mm_nt(wm, wh) + mm_nt(wl, wh) + mm_nt(wm * 0.5, wm)
            total = term if total is None else total + term
        return total

    def oth_sum(s, work):
        total = None
        for j, parts in work:
            for k in parts:
                right = joined(own.at[shared + j, k, s])
                for lhs in range(3 - k):
                    term = mm_nt(joined(oth.at[s, j, lhs]), right)
                    total = term if total is None else total + term
        return total

    def own_products(s):
        return own_sum(s, range(pairs))

    def oth_products(s):
        return oth_sum(s, [(j, (0, 1, 2)) for j in range(shared)])

    def block(body):
        def trip(_, carry):
            body()
            return carry
        lax.fori_loop(orb, orb + 1, trip, 0)

    z_pair = (pl.ds(2 * orb, 2), pl.ds(2 * (1 - orb), 2))

    def put(s, part, block):
        for h in range(2):
            p_buf[s, h, z_pair[part]] = block[:, h * 128:(h + 1) * 128].reshape(2, 4, 4, 8, 128)

    def put_own(s):
        put(s, 0, j_acc[...] - (y_acc[...] + y_acc[...].T))

    def put_oth(s):
        put(s, 1, -(z_f[s] + z_r[s].T))

    def by_core(body, *args):
        for r in range(2):
            @pl.when(orb == r)
            def _():
                body(r, *args)

    dists = (2, 1, 3)

    def line1(axis, zs, where):
        return {0: (where,), 1: (zs, where), 2: (zs, slice(None), where)}[axis]

    def copy1(r, s, h, part, dist):
        axis = ORDERS[r][s][h][0]
        zs = pl.ds(2 * (r if part == 0 else 1 - r), 2)
        device, target = peer(axis, dist)
        dst = r1.at[s, h, dist - 1] if axis == 0 else r1.at[s, h, dist - 1, zs]
        return pltpu.make_async_remote_copy(
            src_ref=p_buf.at[(s, h) + line1(axis, zs, target)], dst_ref=dst,
            send_sem=send1.at[s, h, part, dist - 1], recv_sem=recv1.at[s, h, part, dist - 1],
            device_id=device, device_id_type=MESH)

    def copy2(r, s, h, dist):
        order = ORDERS[r][s][h]
        device, target = peer(order[1], dist)
        where = (target,) if order[1] == min(order[1:]) else (slice(None), target)
        return pltpu.make_async_remote_copy(
            src_ref=s1.at[(s, h) + where], dst_ref=r2.at[s, h, dist - 1],
            send_sem=send2.at[s, h, dist - 1], recv_sem=recv2.at[s, h, dist - 1],
            device_id=device, device_id_type=MESH)

    def copy3(r, s, h, dist):
        device, target = peer(ORDERS[r][s][h][2], dist)
        return pltpu.make_async_remote_copy(
            src_ref=s2.at[s, h, target], dst_ref=r3.at[s, h, dist - 1],
            send_sem=send3.at[s, h, dist - 1], recv_sem=recv3.at[s, h, dist - 1],
            device_id=device, device_id_type=MESH)

    def start1(r, s, part):
        for dist in dists:
            for h in range(2):
                if ORDERS[r][s][h][0] == 0:
                    @pl.when((peer(0, dist)[1] // 2 == r) == (part == 0))
                    def _():
                        copy1(r, s, h, 0, dist).start()
                else:
                    copy1(r, s, h, part, dist).start()

    def parts1(r, s, h):
        return (0,) if ORDERS[r][s][h][0] == 0 else (1, 0)

    def finish1(r, s):
        for h in range(2):
            axis = ORDERS[r][s][h][0]
            for part in parts1(r, s, h):
                for dist in dists:
                    copy1(r, s, h, part, dist).wait_recv()
                zs = pl.ds(2 * (r if part == 0 else 1 - r), 2)
                kept = p_buf[(s, h) + line1(axis, zs, coords[axis])]
                if axis == 0:
                    s1[s, h] = kept + r1[s, h, 0] + r1[s, h, 1] + r1[s, h, 2]
                else:
                    s1[s, h, zs] = kept + r1[s, h, 0, zs] + r1[s, h, 1, zs] + r1[s, h, 2, zs]
            for dist in dists:
                copy2(r, s, h, dist).start()

    def finish2(r, s):
        for h in range(2):
            order = ORDERS[r][s][h]
            for dist in dists:
                copy2(r, s, h, dist).wait_recv()
            where = (coords[order[1]],) if order[1] == min(order[1:]) else (slice(None), coords[order[1]])
            s2[s, h] = s1[(s, h) + where] + r2[s, h, 0] + r2[s, h, 1] + r2[s, h, 2]
            for dist in dists:
                copy3(r, s, h, dist).start()

    def finish3(r, s):
        for h in range(2):
            for dist in dists:
                copy3(r, s, h, dist).wait_recv()
            o_ref[s, :, h * 128:(h + 1) * 128] = (
                s2[s, h, coords[ORDERS[r][s][h][2]]] + r3[s, h, 0] + r3[s, h, 1] + r3[s, h, 2])

    def sent(r):
        for s in range(2):
            for h in range(2):
                for dist in dists:
                    for part in parts1(r, s, h):
                        copy1(r, s, h, part, dist).wait_send()
                    copy2(r, s, h, dist).wait_send()
                    copy3(r, s, h, dist).wait_send()

    def reduce_rest(r):
        for s in range(2):
            finish1(r, s)
        for s in range(2):
            finish2(r, s)
        for s in range(2):
            finish3(r, s)
        sent(r)

    kept = range(shared, pairs)

    def alpha_oth():
        take(0)
        j_t[...] = coulomb(kept, oth_row, half).T
        j_acc[...] = coulomb(kept, own_row, half)
        z_f[0] = oth_products(0) - j_t[...]

    def beta_oth():
        take(1)
        j_acc[...] = coulomb(range(shared), own_row, half, j_acc)
        z_f[1] = oth_products(1) - j_t[...]

    def alpha_own():
        y_acc[...] = own_products(0)

    def beta_own():
        y_acc[...] = own_products(1)

    for p in range(shared):
        t_copy(p).wait_recv()
        g_landed(shared + p)
    block(alpha_oth)
    z_copy(0).start()
    for p in range(shared):
        g_landed(p)
    block(beta_oth)
    z_copy(1).start()
    z_copy(0).wait_recv()
    put_oth(0)
    by_core(start1, 0, 1)
    block(alpha_own)
    put_own(0)
    by_core(start1, 0, 0)
    z_copy(1).wait_recv()
    put_oth(1)
    by_core(start1, 1, 1)
    block(beta_own)
    put_own(1)
    by_core(start1, 1, 0)
    by_core(reduce_rest)
    for p in range(shared):
        t_copy(p).wait_send()
    for p in range(pairs):
        g_copy(p).wait_send()
    for s in range(2):
        z_copy(s).wait_send()


def solution(mesh):
    def local_build(b_local, c_alpha, c_beta):
        n_q, half, rows = b_local.shape
        pairs = n_q // 2
        vmem = pltpu.VMEM
        dma = pltpu.SemaphoreType.DMA
        anywhere = pl.BlockSpec(memory_space=pl.ANY)
        out = pl.pallas_call(
            functools.partial(kernel, n_q, rows),
            out_shape=pltpu.VMEM((2, 8, half), F32),
            in_specs=[anywhere, anywhere, anywhere],
            out_specs=pl.BlockSpec(memory_space=vmem),
            scratch_shapes=[
                vmem((n_q, half, rows), F32),
                vmem((c_alpha.shape[1], rows), F32),
                vmem((c_beta.shape[1], rows), F32),
                vmem((256, rows), F32),
                vmem((rows, 256), F32),
                vmem((3, 2, rows, 128), BF16),
                vmem((pairs, 2, half, 256), F32),
                vmem((pairs // 2, 2, half, 256), F32),
                vmem((pairs, 2, 8, 128), F32),
                vmem((pairs, 2, 8, 128), F32),
                vmem((pairs, 3, 2, 2, half, 128), BF16),
                vmem((2, pairs // 2, 3, 2, half, 128), BF16),
                vmem((half, half), F32),
                vmem((half, half), F32),
                vmem((half, half), F32),
                vmem((2, half, half), F32),
                vmem((2, half, half), F32),
                vmem((2, 2, 4, 4, 4, 8, 128), F32),
                vmem((2, 2, 3, 4, 4, 8, 128), F32),
                vmem((2, 2, 4, 4, 8, 128), F32),
                vmem((2, 2, 3, 4, 8, 128), F32),
                vmem((2, 2, 4, 8, 128), F32),
                vmem((2, 2, 3, 8, 128), F32),
                dma((pairs,)),
                dma((2,)),
                dma((pairs // 2,)),
                dma((pairs // 2,)),
                dma((pairs,)),
                dma((pairs,)),
                dma((2,)),
                dma((2,)),
                dma((2, 2, 2, 3)),
                dma((2, 2, 2, 3)),
                dma((2, 2, 3)),
                dma((2, 2, 3)),
                dma((2, 2, 3)),
                dma((2, 2, 3)),
            ],
            compiler_params=pltpu.CompilerParams(
                collective_id=0, has_side_effects=True, vmem_limit_bytes=60 * 1024 * 1024),
        )(b_local, c_alpha.T, c_beta.T)
        return out[0].T, out[1].T

    spec_b = P(("sys", "aux"), "orb", None)
    spec_c = P("sys", None)
    spec_g = P(("sys", "orb"), "aux")
    return jax.shard_map(local_build, mesh=mesh, in_specs=(spec_b, spec_c, spec_c), out_specs=(spec_g, spec_g), check_vma=False)
```

```python
import functools

import jax
import jax.numpy as jnp
from jax import lax
from jax.experimental import pallas as pl
from jax.experimental.pallas import tpu as pltpu
from jax.sharding import PartitionSpec as P

MESH = pl.DeviceIdType.MESH
F32 = jnp.float32
BF16 = jnp.bfloat16
NT = (((1,), (1,)), ((), ()))
T_BLOCKS = (1, 4, 5)
X_FIRST, Y_FIRST, Z_FIRST = (2, 0, 1), (1, 0, 2), (0, 1, 2)
ORDERS = (((Z_FIRST, X_FIRST), (X_FIRST, Y_FIRST)), ((Y_FIRST, X_FIRST), (Z_FIRST, Y_FIRST)))


def split3(value):
    high = value.astype(BF16)
    rest = value - high.astype(F32)
    mid = rest.astype(BF16)
    low = (rest - mid.astype(F32)).astype(BF16)
    return high, mid, low


def mm(a, b):
    return jnp.dot(a, b, preferred_element_type=F32)


def mm_nt(a, b):
    return lax.dot_general(a, b, NT, preferred_element_type=F32)


def joined(ref):
    return jnp.concatenate([ref[i] for i in range(ref.shape[0])], axis=1)


def kernel(n_q, rows, *refs):
    (b_ref, ca_ref, cb_ref, o_ref, b_v, ca_v, cb_v, c_pad, c_f, c_s, t_f, t_r, g_f, g_r, own, oth, j_acc, z_f, z_r,
     p_buf, r1, s1, r2, s2, r3, b_sem, c_sem, t_send, t_recv, g_send, g_recv, z_send, z_recv,
     send1, recv1, send2, recv2, send3, recv3) = refs
    pairs = n_q // 2
    shared = pairs // 2
    half = rows // 2
    aux = lax.axis_index("aux")
    orb = lax.axis_index("orb")
    coords = (aux // 16, lax.rem(aux // 4, 4), lax.rem(aux, 4))
    strides = (16, 4, 1)
    partner = {"aux": aux, "orb": 1 - orb}

    def peer(axis, dist):
        target = lax.rem(coords[axis] + dist, 4)
        return {"aux": aux + (target - coords[axis]) * strides[axis], "orb": orb}, target

    def b_copy(p):
        first = shared * (1 - orb)
        where = lax.rem(p + first, pairs)
        return pltpu.make_async_copy(b_ref.at[pl.ds(2 * where, 2)], b_v.at[pl.ds(2 * p, 2)], b_sem.at[p])

    c_copies = (pltpu.make_async_copy(ca_ref, ca_v, c_sem.at[0]), pltpu.make_async_copy(cb_ref, cb_v, c_sem.at[1]))
    for copy in c_copies:
        copy.start()
    for p in range(T_BLOCKS[0] + T_BLOCKS[1]):
        b_copy(p).start()

    barrier = pltpu.get_barrier_semaphore()
    pl.semaphore_signal(barrier, inc=1, device_id=partner, device_id_type=MESH)
    for axis in range(3):
        for dist in (1, 2, 3):
            pl.semaphore_signal(barrier, inc=1, device_id=peer(axis, dist)[0], device_id_type=MESH)

    c_pad[...] = jnp.zeros_like(c_pad)
    for copy in c_copies:
        copy.wait()
    c_pad[0:ca_v.shape[0], :] = ca_v[...]
    c_pad[128:128 + cb_v.shape[0], :] = cb_v[...]
    c_all = c_pad[...].T
    c_f[...] = c_all
    for k, part in enumerate(split3(c_all)):
        c_s[k, 0] = part[:, 0:128]
        c_s[k, 1] = part[:, 128:256]
    own_row = pl.multiple_of(orb * half, half)
    oth_row = pl.multiple_of((1 - orb) * half, half)

    def t_copy(p):
        return pltpu.make_async_remote_copy(
            src_ref=t_f.at[p], dst_ref=t_r.at[p], send_sem=t_send.at[p], recv_sem=t_recv.at[p],
            device_id=partner, device_id_type=MESH)

    def g_copy(p):
        there = lax.rem(p + shared, pairs)
        return pltpu.make_async_remote_copy(
            src_ref=g_f.at[p], dst_ref=g_r.at[there], send_sem=g_send.at[p], recv_sem=g_recv.at[there],
            device_id=partner, device_id_type=MESH)

    def g_landed(p):
        g_copy(lax.rem(p + shared, pairs)).wait_recv()

    def z_copy(s):
        return pltpu.make_async_remote_copy(
            src_ref=z_f.at[s], dst_ref=z_r.at[s], send_sem=z_send.at[s], recv_sem=z_recv.at[s],
            device_id=partner, device_id_type=MESH)

    def t_step(p):
        for e in range(2):
            h, m, l = split3(b_v[2 * p + e])
            ch, cm, cl = joined(c_s.at[0]), joined(c_s.at[1]), joined(c_s.at[2])
            t = mm(h, ch) + mm(m, ch) + mm(l, ch) + mm(h, cm) + mm(m, cm) + mm(h, cl)
            t_f[p, e] = t
            prod = (t * c_f[pl.ds(own_row, half), :]).reshape(half // 8, 8, 256).sum(axis=0)
            g_f[p, e] = prod[:, 0:128] + prod[:, 128:256]
            for k, part in enumerate(split3(t)):
                for s in range(2):
                    own[p, k, s, e] = part[:, s * 128:(s + 1) * 128]

    def send_t(p):
        g_copy(p).start()

        if p < shared:
            t_copy(p).start()

    start = 0
    for i, size in enumerate(T_BLOCKS):
        ps = range(start, start + size)
        start += size
        for p in ps:
            b_copy(p).wait()
        if i == 0:
            for p in range(T_BLOCKS[0] + T_BLOCKS[1], pairs):
                b_copy(p).start()
        for p in ps:
            t_step(p)
        if i == 0:
            pl.semaphore_wait(barrier, 10)
        for p in ps:
            send_t(p)

    def take(s):
        for j in range(shared):
            for e in range(2):
                for k, part in enumerate(split3(t_r[j, e, :, s * 128:(s + 1) * 128])):
                    oth[s, j, k, e] = part

    def coulomb(ps, cols, width, old=None):
        qs = [(p, e) for p in ps for e in range(2)]
        g = [jnp.sum(g_f[q] + g_r[q]) for q in qs]
        out = []
        for row in range(0, half, 8):
            total = None if old is None else old[row:row + 8, :]
            for gq, (p, e) in zip(g, qs):
                term = gq * b_v[2 * p + e, row:row + 8, pl.ds(cols, width)]
                total = term if total is None else total + term
            out.append(total)
        return jnp.concatenate(out, axis=0)

    def own_sum(s, ps):
        total = None
        for p in ps:
            wh, wm, wl = (joined(own.at[p, k, s]) for k in range(3))
            term = mm_nt(wh * 0.5, wh) + mm_nt(wm, wh) + mm_nt(wl, wh) + mm_nt(wm * 0.5, wm)
            total = term if total is None else total + term
        return total

    def oth_sum(s, work):
        total = None
        for j, parts in work:
            for k in parts:
                right = joined(own.at[shared + j, k, s])
                for lhs in range(3 - k):
                    term = mm_nt(joined(oth.at[s, j, lhs]), right)
                    total = term if total is None else total + term
        return total

    def own_products(s):
        return own_sum(s, range(pairs))

    def oth_products(s):
        return oth_sum(s, [(j, (0, 1, 2)) for j in range(shared)])

    def block(body):
        def trip(_, carry):
            body()
            return carry
        lax.fori_loop(orb, orb + 1, trip, 0)

    z_pair = (pl.ds(2 * orb, 2), pl.ds(2 * (1 - orb), 2))

    def put(s, part, block):
        for h in range(2):
            p_buf[s, h, z_pair[part]] = block[:, h * 128:(h + 1) * 128].reshape(2, 4, 4, 8, 128)

    def put_oth(s):
        put(s, 1, -(z_f[s] + z_r[s].T))

    def by_core(body, *args):
        for r in range(2):
            @pl.when(orb == r)
            def _():
                body(r, *args)

    dists = (2, 1, 3)

    def line1(axis, zs, where):
        return {0: (where,), 1: (zs, where), 2: (zs, slice(None), where)}[axis]

    def copy1(r, s, h, part, dist):
        axis = ORDERS[r][s][h][0]
        zs = pl.ds(2 * (r if part == 0 else 1 - r), 2)
        device, target = peer(axis, dist)
        dst = r1.at[s, h, dist - 1] if axis == 0 else r1.at[s, h, dist - 1, zs]
        return pltpu.make_async_remote_copy(
            src_ref=p_buf.at[(s, h) + line1(axis, zs, target)], dst_ref=dst,
            send_sem=send1.at[s, h, part, dist - 1], recv_sem=recv1.at[s, h, part, dist - 1],
            device_id=device, device_id_type=MESH)

    def copy2(r, s, h, dist):
        order = ORDERS[r][s][h]
        device, target = peer(order[1], dist)
        where = (target,) if order[1] == min(order[1:]) else (slice(None), target)
        return pltpu.make_async_remote_copy(
            src_ref=s1.at[(s, h) + where], dst_ref=r2.at[s, h, dist - 1],
            send_sem=send2.at[s, h, dist - 1], recv_sem=recv2.at[s, h, dist - 1],
            device_id=device, device_id_type=MESH)

    def copy3(r, s, h, dist):
        device, target = peer(ORDERS[r][s][h][2], dist)
        return pltpu.make_async_remote_copy(
            src_ref=s2.at[s, h, target], dst_ref=r3.at[s, h, dist - 1],
            send_sem=send3.at[s, h, dist - 1], recv_sem=recv3.at[s, h, dist - 1],
            device_id=device, device_id_type=MESH)

    def start1(r, s, part):
        for dist in dists:
            for h in range(2):
                if ORDERS[r][s][h][0] == 0:
                    @pl.when((peer(0, dist)[1] // 2 == r) == (part == 0))
                    def _():
                        copy1(r, s, h, 0, dist).start()
                else:
                    copy1(r, s, h, part, dist).start()

    def parts1(r, s, h):
        return (0,) if ORDERS[r][s][h][0] == 0 else (1, 0)

    def finish1(r, s):
        for h in range(2):
            axis = ORDERS[r][s][h][0]
            for part in parts1(r, s, h):
                for dist in dists:
                    copy1(r, s, h, part, dist).wait_recv()
                zs = pl.ds(2 * (r if part == 0 else 1 - r), 2)
                kept = p_buf[(s, h) + line1(axis, zs, coords[axis])]
                if axis == 0:
                    s1[s, h] = kept + r1[s, h, 0] + r1[s, h, 1] + r1[s, h, 2]
                else:
                    s1[s, h, zs] = kept + r1[s, h, 0, zs] + r1[s, h, 1, zs] + r1[s, h, 2, zs]
            for dist in dists:
                copy2(r, s, h, dist).start()

    def finish2(r, s):
        for h in range(2):
            order = ORDERS[r][s][h]
            for dist in dists:
                copy2(r, s, h, dist).wait_recv()
            where = (coords[order[1]],) if order[1] == min(order[1:]) else (slice(None), coords[order[1]])
            s2[s, h] = s1[(s, h) + where] + r2[s, h, 0] + r2[s, h, 1] + r2[s, h, 2]
            for dist in dists:
                copy3(r, s, h, dist).start()

    def finish3(r, s):
        for h in range(2):
            for dist in dists:
                copy3(r, s, h, dist).wait_recv()
            o_ref[s, :, h * 128:(h + 1) * 128] = (
                s2[s, h, coords[ORDERS[r][s][h][2]]] + r3[s, h, 0] + r3[s, h, 1] + r3[s, h, 2])

    def sent(r, s, phase):
        for h in range(2):
            for dist in dists:
                if phase == 0:
                    for part in parts1(r, s, h):
                        copy1(r, s, h, part, dist).wait_send()
                else:
                    (copy2, copy3)[phase - 1](r, s, h, dist).wait_send()

    def reduce_rest(r):
        for phase, finish in enumerate((finish1, finish2, finish3)):
            if phase == 2:
                for s in range(2):
                    sent(r, s, 2)
            for s in range(2):
                finish(r, s)
                if phase < 2:
                    sent(r, s, phase)

    kept = range(shared, pairs)

    def oth_block():
        for s in range(2):
            take(s)
        off = coulomb(kept, oth_row, half).T
        j_acc[...] = coulomb(kept, own_row, half)
        for s in range(2):
            z_f[s] = oth_products(s) - off

    def alpha_block():
        j_own = coulomb(range(shared), own_row, half, j_acc)
        j_acc[...] = j_own
        y = own_products(0)
        put(0, 0, j_own - (y + y.T))

    def beta_block():
        y = own_products(1)
        put(1, 0, j_acc[...] - (y + y.T))

    for p in range(shared):
        t_copy(p).wait_recv()
        g_landed(shared + p)
    block(oth_block)
    for s in range(2):
        z_copy(s).start()
    for p in range(shared):
        g_landed(p)
    block(alpha_block)
    by_core(start1, 0, 0)
    for s in range(2):
        z_copy(s).wait_recv()
        put_oth(s)
    by_core(start1, 0, 1)
    by_core(start1, 1, 1)
    block(beta_block)
    by_core(start1, 1, 0)
    for p in range(shared):
        t_copy(p).wait_send()
    for p in range(pairs):
        g_copy(p).wait_send()
    for s in range(2):
        z_copy(s).wait_send()
    by_core(reduce_rest)


def solution(mesh):
    def local_build(b_local, c_alpha, c_beta):
        n_q, half, rows = b_local.shape
        pairs = n_q // 2
        vmem = pltpu.VMEM
        dma = pltpu.SemaphoreType.DMA
        anywhere = pl.BlockSpec(memory_space=pl.ANY)
        out = pl.pallas_call(
            functools.partial(kernel, n_q, rows),
            out_shape=pltpu.VMEM((2, 8, half), F32),
            in_specs=[anywhere, anywhere, anywhere],
            out_specs=pl.BlockSpec(memory_space=vmem),
            scratch_shapes=[
                vmem((n_q, half, rows), F32),
                vmem((c_alpha.shape[1], rows), F32),
                vmem((c_beta.shape[1], rows), F32),
                vmem((256, rows), F32),
                vmem((rows, 256), F32),
                vmem((3, 2, rows, 128), BF16),
                vmem((pairs, 2, half, 256), F32),
                vmem((pairs // 2, 2, half, 256), F32),
                vmem((pairs, 2, 8, 128), F32),
                vmem((pairs, 2, 8, 128), F32),
                vmem((pairs, 3, 2, 2, half, 128), BF16),
                vmem((2, pairs // 2, 3, 2, half, 128), BF16),
                vmem((half, half), F32),
                vmem((2, half, half), F32),
                vmem((2, half, half), F32),
                vmem((2, 2, 4, 4, 4, 8, 128), F32),
                vmem((2, 2, 3, 4, 4, 8, 128), F32),
                vmem((2, 2, 4, 4, 8, 128), F32),
                vmem((2, 2, 3, 4, 8, 128), F32),
                vmem((2, 2, 4, 8, 128), F32),
                vmem((2, 2, 3, 8, 128), F32),
                dma((pairs,)),
                dma((2,)),
                dma((pairs // 2,)),
                dma((pairs // 2,)),
                dma((pairs,)),
                dma((pairs,)),
                dma((2,)),
                dma((2,)),
                dma((2, 2, 2, 3)),
                dma((2, 2, 2, 3)),
                dma((2, 2, 3)),
                dma((2, 2, 3)),
                dma((2, 2, 3)),
                dma((2, 2, 3)),
            ],
            compiler_params=pltpu.CompilerParams(
                collective_id=0, has_side_effects=True, vmem_limit_bytes=60 * 1024 * 1024),
        )(b_local, c_alpha.T, c_beta.T)
        return out[0].T, out[1].T

    spec_b = P(("sys", "aux"), "orb", None)
    spec_c = P("sys", None)
    spec_g = P(("sys", "orb"), "aux")
    return jax.shard_map(local_build, mesh=mesh, in_specs=(spec_b, spec_c, spec_c), out_specs=(spec_g, spec_g), check_vma=False)
```

```python
import functools

import jax
import jax.numpy as jnp
from jax import lax
from jax.experimental import pallas as pl
from jax.experimental.pallas import tpu as pltpu
from jax.sharding import PartitionSpec as P

MESH = pl.DeviceIdType.MESH
F32 = jnp.float32
BF16 = jnp.bfloat16
NT = (((1,), (1,)), ((), ()))
T_BLOCKS = (1, 4, 5)
X_FIRST, Y_FIRST, Z_FIRST = (2, 0, 1), (1, 0, 2), (0, 1, 2)
ORDERS = (((Z_FIRST, X_FIRST), (X_FIRST, Y_FIRST)), ((Y_FIRST, X_FIRST), (Z_FIRST, Y_FIRST)))


def split3(value):
    high = value.astype(BF16)
    rest = value - high.astype(F32)
    mid = rest.astype(BF16)
    low = (rest - mid.astype(F32)).astype(BF16)
    return high, mid, low


def mm(a, b):
    return jnp.dot(a, b, preferred_element_type=F32)


def mm_nt(a, b):
    return lax.dot_general(a, b, NT, preferred_element_type=F32)


def joined(ref):
    return jnp.concatenate([ref[i] for i in range(ref.shape[0])], axis=1)


def kernel(n_q, rows, *refs):
    (b_ref, ca_ref, cb_ref, o_ref, b_v, ca_v, cb_v, c_pad, c_f, c_s, t_f, t_r, g_f, g_r, own, oth, j_acc, j_t, z_f, z_r,
     p_buf, r1, s1, r2, s2, r3, b_sem, c_sem, t_send, t_recv, g_send, g_recv, z_send, z_recv,
     send1, recv1, send2, recv2, send3, recv3) = refs
    pairs = n_q // 2
    shared = pairs // 2
    half = rows // 2
    aux = lax.axis_index("aux")
    orb = lax.axis_index("orb")
    coords = (aux // 16, lax.rem(aux // 4, 4), lax.rem(aux, 4))
    strides = (16, 4, 1)
    partner = {"aux": aux, "orb": 1 - orb}

    def peer(axis, dist):
        target = lax.rem(coords[axis] + dist, 4)
        return {"aux": aux + (target - coords[axis]) * strides[axis], "orb": orb}, target

    def b_copy(p):
        first = shared * (1 - orb)
        where = lax.rem(p + first, pairs)
        return pltpu.make_async_copy(b_ref.at[pl.ds(2 * where, 2)], b_v.at[pl.ds(2 * p, 2)], b_sem.at[p])

    c_copies = (pltpu.make_async_copy(ca_ref, ca_v, c_sem.at[0]), pltpu.make_async_copy(cb_ref, cb_v, c_sem.at[1]))
    for copy in c_copies:
        copy.start()
    for p in range(T_BLOCKS[0] + T_BLOCKS[1]):
        b_copy(p).start()

    barrier = pltpu.get_barrier_semaphore()
    pl.semaphore_signal(barrier, inc=1, device_id=partner, device_id_type=MESH)
    for axis in range(3):
        for dist in (1, 2, 3):
            pl.semaphore_signal(barrier, inc=1, device_id=peer(axis, dist)[0], device_id_type=MESH)

    c_pad[...] = jnp.zeros_like(c_pad)
    for copy in c_copies:
        copy.wait()
    c_pad[0:ca_v.shape[0], :] = ca_v[...]
    c_pad[128:128 + cb_v.shape[0], :] = cb_v[...]
    c_all = c_pad[...].T
    c_f[...] = c_all
    for k, part in enumerate(split3(c_all)):
        c_s[k, 0] = part[:, 0:128]
        c_s[k, 1] = part[:, 128:256]
    own_row = pl.multiple_of(orb * half, half)
    oth_row = pl.multiple_of((1 - orb) * half, half)

    def t_copy(p):
        return pltpu.make_async_remote_copy(
            src_ref=t_f.at[p], dst_ref=t_r.at[p], send_sem=t_send.at[p], recv_sem=t_recv.at[p],
            device_id=partner, device_id_type=MESH)

    def g_copy(p):
        there = lax.rem(p + shared, pairs)
        return pltpu.make_async_remote_copy(
            src_ref=g_f.at[p], dst_ref=g_r.at[there], send_sem=g_send.at[p], recv_sem=g_recv.at[there],
            device_id=partner, device_id_type=MESH)

    def g_landed(p):
        g_copy(lax.rem(p + shared, pairs)).wait_recv()

    def z_copy(s):
        return pltpu.make_async_remote_copy(
            src_ref=z_f.at[s], dst_ref=z_r.at[s], send_sem=z_send.at[s], recv_sem=z_recv.at[s],
            device_id=partner, device_id_type=MESH)

    def t_step(p):
        for e in range(2):
            h, m, l = split3(b_v[2 * p + e])
            ch, cm, cl = joined(c_s.at[0]), joined(c_s.at[1]), joined(c_s.at[2])
            t = mm(h, ch) + mm(m, ch) + mm(l, ch) + mm(h, cm) + mm(m, cm) + mm(h, cl)
            t_f[p, e] = t
            prod = (t * c_f[pl.ds(own_row, half), :]).reshape(half // 8, 8, 256).sum(axis=0)
            g_f[p, e] = prod[:, 0:128] + prod[:, 128:256]
            for k, part in enumerate(split3(t)):
                for s in range(2):
                    own[p, k, s, e] = part[:, s * 128:(s + 1) * 128]

    def send_t(p):
        g_copy(p).start()

        if p < shared:
            t_copy(p).start()

    start = 0
    for i, size in enumerate(T_BLOCKS):
        ps = range(start, start + size)
        start += size
        for p in ps:
            b_copy(p).wait()
        if i == 0:
            for p in range(T_BLOCKS[0] + T_BLOCKS[1], pairs):
                b_copy(p).start()
        for p in ps:
            t_step(p)
        if i == 0:
            pl.semaphore_wait(barrier, 10)
        for p in ps:
            send_t(p)

    def take(s):
        for j in range(shared):
            for e in range(2):
                for k, part in enumerate(split3(t_r[j, e, :, s * 128:(s + 1) * 128])):
                    oth[s, j, k, e] = part

    def coulomb(ps, cols, width, old=None):
        qs = [(p, e) for p in ps for e in range(2)]
        g = [jnp.sum(g_f[q] + g_r[q]) for q in qs]
        out = []
        for row in range(0, half, 8):
            total = None if old is None else old[row:row + 8, :]
            for gq, (p, e) in zip(g, qs):
                term = gq * b_v[2 * p + e, row:row + 8, pl.ds(cols, width)]
                total = term if total is None else total + term
            out.append(total)
        return jnp.concatenate(out, axis=0)

    def own_sum(s, ps):
        total = None
        for p in ps:
            wh, wm, wl = (joined(own.at[p, k, s]) for k in range(3))
            term = mm_nt(wh * 0.5, wh) + mm_nt(wm, wh) + mm_nt(wl, wh) + mm_nt(wm * 0.5, wm)
            total = term if total is None else total + term
        return total

    def oth_sum(s, work):
        total = None
        for j, parts in work:
            for k in parts:
                right = joined(own.at[shared + j, k, s])
                for lhs in range(3 - k):
                    term = mm_nt(joined(oth.at[s, j, lhs]), right)
                    total = term if total is None else total + term
        return total

    def own_products(s):
        return own_sum(s, range(pairs))

    def oth_products(s):
        return oth_sum(s, [(j, (0, 1, 2)) for j in range(shared)])

    def block(body):
        def trip(_, carry):
            body()
            return carry
        lax.fori_loop(orb, orb + 1, trip, 0)

    z_pair = (pl.ds(2 * orb, 2), pl.ds(2 * (1 - orb), 2))

    def put(s, part, block):
        for h in range(2):
            p_buf[s, h, z_pair[part]] = block[:, h * 128:(h + 1) * 128].reshape(2, 4, 4, 8, 128)

    def put_oth(s):
        put(s, 1, -(z_f[s] + z_r[s].T))

    def by_core(body, *args):
        for r in range(2):
            @pl.when(orb == r)
            def _():
                body(r, *args)

    dists = (2, 1, 3)

    def line1(axis, zs, where):
        return {0: (where,), 1: (zs, where), 2: (zs, slice(None), where)}[axis]

    def copy1(r, s, h, part, dist):
        axis = ORDERS[r][s][h][0]
        zs = pl.ds(2 * (r if part == 0 else 1 - r), 2)
        device, target = peer(axis, dist)
        dst = r1.at[s, h, dist - 1] if axis == 0 else r1.at[s, h, dist - 1, zs]
        return pltpu.make_async_remote_copy(
            src_ref=p_buf.at[(s, h) + line1(axis, zs, target)], dst_ref=dst,
            send_sem=send1.at[s, h, part, dist - 1], recv_sem=recv1.at[s, h, part, dist - 1],
            device_id=device, device_id_type=MESH)

    def copy2(r, s, h, dist):
        order = ORDERS[r][s][h]
        device, target = peer(order[1], dist)
        where = (target,) if order[1] == min(order[1:]) else (slice(None), target)
        return pltpu.make_async_remote_copy(
            src_ref=s1.at[(s, h) + where], dst_ref=r2.at[s, h, dist - 1],
            send_sem=send2.at[s, h, dist - 1], recv_sem=recv2.at[s, h, dist - 1],
            device_id=device, device_id_type=MESH)

    def copy3(r, s, h, dist):
        device, target = peer(ORDERS[r][s][h][2], dist)
        return pltpu.make_async_remote_copy(
            src_ref=s2.at[s, h, target], dst_ref=r3.at[s, h, dist - 1],
            send_sem=send3.at[s, h, dist - 1], recv_sem=recv3.at[s, h, dist - 1],
            device_id=device, device_id_type=MESH)

    def start1(r, s, part):
        for dist in dists:
            for h in range(2):
                if ORDERS[r][s][h][0] == 0:
                    @pl.when((peer(0, dist)[1] // 2 == r) == (part == 0))
                    def _():
                        copy1(r, s, h, 0, dist).start()
                else:
                    copy1(r, s, h, part, dist).start()

    def parts1(r, s, h):
        return (0,) if ORDERS[r][s][h][0] == 0 else (1, 0)

    def finish1(r, s):
        for h in range(2):
            axis = ORDERS[r][s][h][0]
            for part in parts1(r, s, h):
                for dist in dists:
                    copy1(r, s, h, part, dist).wait_recv()
                zs = pl.ds(2 * (r if part == 0 else 1 - r), 2)
                kept = p_buf[(s, h) + line1(axis, zs, coords[axis])]
                if axis == 0:
                    s1[s, h] = kept + r1[s, h, 0] + r1[s, h, 1] + r1[s, h, 2]
                else:
                    s1[s, h, zs] = kept + r1[s, h, 0, zs] + r1[s, h, 1, zs] + r1[s, h, 2, zs]
            for dist in dists:
                copy2(r, s, h, dist).start()

    def finish2(r, s):
        for h in range(2):
            order = ORDERS[r][s][h]
            for dist in dists:
                copy2(r, s, h, dist).wait_recv()
            where = (coords[order[1]],) if order[1] == min(order[1:]) else (slice(None), coords[order[1]])
            s2[s, h] = s1[(s, h) + where] + r2[s, h, 0] + r2[s, h, 1] + r2[s, h, 2]
            for dist in dists:
                copy3(r, s, h, dist).start()

    def finish3(r, s):
        for h in range(2):
            for dist in dists:
                copy3(r, s, h, dist).wait_recv()
            o_ref[s, :, h * 128:(h + 1) * 128] = (
                s2[s, h, coords[ORDERS[r][s][h][2]]] + r3[s, h, 0] + r3[s, h, 1] + r3[s, h, 2])

    def sent(r, s, phase):
        for h in range(2):
            for dist in dists:
                if phase == 0:
                    for part in parts1(r, s, h):
                        copy1(r, s, h, part, dist).wait_send()
                else:
                    (copy2, copy3)[phase - 1](r, s, h, dist).wait_send()

    def reduce_rest(r):
        for phase, finish in enumerate((finish1, finish2, finish3)):
            if phase == 2:
                for s in range(2):
                    sent(r, s, 2)
            for s in range(2):
                finish(r, s)
                if phase < 2:
                    sent(r, s, phase)

    kept = range(shared, pairs)

    def alpha_oth():
        take(0)
        j_t[...] = coulomb(kept, oth_row, half).T
        j_acc[...] = coulomb(kept, own_row, half)
        z_f[0] = oth_products(0) - j_t[...]

    def beta_oth():
        take(1)
        j_acc[...] = coulomb(range(shared), own_row, half, j_acc)
        z_f[1] = oth_products(1) - j_t[...]

    def own_block(s):
        y = own_products(s)
        put(s, 0, j_acc[...] - (y + y.T))

    for p in range(shared):
        t_copy(p).wait_recv()
        g_landed(shared + p)
    block(alpha_oth)
    z_copy(0).start()
    for p in range(shared):
        g_landed(p)
    block(beta_oth)
    z_copy(1).start()
    z_copy(0).wait_recv()
    put_oth(0)
    by_core(start1, 0, 1)
    block(functools.partial(own_block, 0))
    by_core(start1, 0, 0)
    z_copy(1).wait_recv()
    put_oth(1)
    by_core(start1, 1, 1)
    block(functools.partial(own_block, 1))
    by_core(start1, 1, 0)
    for p in range(shared):
        t_copy(p).wait_send()
    for p in range(pairs):
        g_copy(p).wait_send()
    for s in range(2):
        z_copy(s).wait_send()
    by_core(reduce_rest)


def solution(mesh):
    def local_build(b_local, c_alpha, c_beta):
        n_q, half, rows = b_local.shape
        pairs = n_q // 2
        vmem = pltpu.VMEM
        dma = pltpu.SemaphoreType.DMA
        anywhere = pl.BlockSpec(memory_space=pl.ANY)
        out = pl.pallas_call(
            functools.partial(kernel, n_q, rows),
            out_shape=pltpu.VMEM((2, 8, half), F32),
            in_specs=[anywhere, anywhere, anywhere],
            out_specs=pl.BlockSpec(memory_space=vmem),
            scratch_shapes=[
                vmem((n_q, half, rows), F32),
                vmem((c_alpha.shape[1], rows), F32),
                vmem((c_beta.shape[1], rows), F32),
                vmem((256, rows), F32),
                vmem((rows, 256), F32),
                vmem((3, 2, rows, 128), BF16),
                vmem((pairs, 2, half, 256), F32),
                vmem((pairs // 2, 2, half, 256), F32),
                vmem((pairs, 2, 8, 128), F32),
                vmem((pairs, 2, 8, 128), F32),
                vmem((pairs, 3, 2, 2, half, 128), BF16),
                vmem((2, pairs // 2, 3, 2, half, 128), BF16),
                vmem((half, half), F32),
                vmem((half, half), F32),
                vmem((2, half, half), F32),
                vmem((2, half, half), F32),
                vmem((2, 2, 4, 4, 4, 8, 128), F32),
                vmem((2, 2, 3, 4, 4, 8, 128), F32),
                vmem((2, 2, 4, 4, 8, 128), F32),
                vmem((2, 2, 3, 4, 8, 128), F32),
                vmem((2, 2, 4, 8, 128), F32),
                vmem((2, 2, 3, 8, 128), F32),
                dma((pairs,)),
                dma((2,)),
                dma((pairs // 2,)),
                dma((pairs // 2,)),
                dma((pairs,)),
                dma((pairs,)),
                dma((2,)),
                dma((2,)),
                dma((2, 2, 2, 3)),
                dma((2, 2, 2, 3)),
                dma((2, 2, 3)),
                dma((2, 2, 3)),
                dma((2, 2, 3)),
                dma((2, 2, 3)),
            ],
            compiler_params=pltpu.CompilerParams(
                collective_id=0, has_side_effects=True, vmem_limit_bytes=60 * 1024 * 1024),
        )(b_local, c_alpha.T, c_beta.T)
        return out[0].T, out[1].T

    spec_b = P(("sys", "aux"), "orb", None)
    spec_c = P("sys", None)
    spec_g = P(("sys", "orb"), "aux")
    return jax.shard_map(local_build, mesh=mesh, in_specs=(spec_b, spec_c, spec_c), out_specs=(spec_g, spec_g), check_vma=False)
```

```python
import functools

import jax
import jax.numpy as jnp
from jax import lax
from jax.experimental import pallas as pl
from jax.experimental.pallas import tpu as pltpu
from jax.sharding import PartitionSpec as P

MESH = pl.DeviceIdType.MESH
F32 = jnp.float32
BF16 = jnp.bfloat16
NT = (((1,), (1,)), ((), ()))
T_BLOCKS = (1, 4, 5)
X_FIRST, Y_FIRST, Z_FIRST = (2, 0, 1), (1, 0, 2), (0, 1, 2)
ORDERS = (((Z_FIRST, X_FIRST), (X_FIRST, Y_FIRST)), ((Y_FIRST, X_FIRST), (Z_FIRST, Y_FIRST)))


def split3(value):
    high = value.astype(BF16)
    rest = value - high.astype(F32)
    mid = rest.astype(BF16)
    low = (rest - mid.astype(F32)).astype(BF16)
    return high, mid, low


def mm(a, b):
    return jnp.dot(a, b, preferred_element_type=F32)


def mm_nt(a, b):
    return lax.dot_general(a, b, NT, preferred_element_type=F32)


def joined(ref):
    return jnp.concatenate([ref[i] for i in range(ref.shape[0])], axis=1)


def kernel(n_q, rows, *refs):
    (b_ref, ca_ref, cb_ref, o_ref, b_v, ca_v, cb_v, c_pad, c_f, c_s, t_f, t_r, g_f, g_r, own, oth, j_acc, j_t, z_f, z_t, z_r,
     p_buf, r1, s1, r2, s2, r3, b_sem, c_sem, t_send, t_recv, g_send, g_recv, z_send, z_recv,
     send1, recv1, send2, recv2, send3, recv3) = refs
    pairs = n_q // 2
    shared = pairs // 2
    half = rows // 2
    aux = lax.axis_index("aux")
    orb = lax.axis_index("orb")
    coords = (aux // 16, lax.rem(aux // 4, 4), lax.rem(aux, 4))
    strides = (16, 4, 1)
    partner = {"aux": aux, "orb": 1 - orb}

    def peer(axis, dist):
        target = lax.rem(coords[axis] + dist, 4)
        return {"aux": aux + (target - coords[axis]) * strides[axis], "orb": orb}, target

    def b_copy(p):
        first = shared * (1 - orb)
        where = lax.rem(p + first, pairs)
        return pltpu.make_async_copy(b_ref.at[pl.ds(2 * where, 2)], b_v.at[pl.ds(2 * p, 2)], b_sem.at[p])

    c_copies = (pltpu.make_async_copy(ca_ref, ca_v, c_sem.at[0]), pltpu.make_async_copy(cb_ref, cb_v, c_sem.at[1]))
    for copy in c_copies:
        copy.start()
    for p in range(T_BLOCKS[0] + T_BLOCKS[1]):
        b_copy(p).start()

    barrier = pltpu.get_barrier_semaphore()
    pl.semaphore_signal(barrier, inc=1, device_id=partner, device_id_type=MESH)
    for axis in range(3):
        for dist in (1, 2, 3):
            pl.semaphore_signal(barrier, inc=1, device_id=peer(axis, dist)[0], device_id_type=MESH)

    c_pad[...] = jnp.zeros_like(c_pad)
    for copy in c_copies:
        copy.wait()
    c_pad[0:ca_v.shape[0], :] = ca_v[...]
    c_pad[128:128 + cb_v.shape[0], :] = cb_v[...]
    c_all = c_pad[...].T
    c_f[...] = c_all
    for k, part in enumerate(split3(c_all)):
        c_s[k, 0] = part[:, 0:128]
        c_s[k, 1] = part[:, 128:256]
    own_row = pl.multiple_of(orb * half, half)
    oth_row = pl.multiple_of((1 - orb) * half, half)

    def t_copy(p):
        return pltpu.make_async_remote_copy(
            src_ref=t_f.at[p], dst_ref=t_r.at[p], send_sem=t_send.at[p], recv_sem=t_recv.at[p],
            device_id=partner, device_id_type=MESH)

    def g_copy(p):
        there = lax.rem(p + shared, pairs)
        return pltpu.make_async_remote_copy(
            src_ref=g_f.at[p], dst_ref=g_r.at[there], send_sem=g_send.at[p], recv_sem=g_recv.at[there],
            device_id=partner, device_id_type=MESH)

    def g_landed(p):
        g_copy(lax.rem(p + shared, pairs)).wait_recv()

    def z_copy(s):
        return pltpu.make_async_remote_copy(
            src_ref=z_t.at[s], dst_ref=z_r.at[s], send_sem=z_send.at[s], recv_sem=z_recv.at[s],
            device_id=partner, device_id_type=MESH)

    def t_step(p):
        for e in range(2):
            h, m, l = split3(b_v[2 * p + e])
            ch, cm, cl = joined(c_s.at[0]), joined(c_s.at[1]), joined(c_s.at[2])
            t = mm(h, ch) + mm(m, ch) + mm(l, ch) + mm(h, cm) + mm(m, cm) + mm(h, cl)
            t_f[p, e] = t
            prod = (t * c_f[pl.ds(own_row, half), :]).reshape(half // 8, 8, 256).sum(axis=0)
            g_f[p, e] = prod[:, 0:128] + prod[:, 128:256]
            for k, part in enumerate(split3(t)):
                for s in range(2):
                    own[p, k, s, e] = part[:, s * 128:(s + 1) * 128]

    def send_t(p):
        g_copy(p).start()

        if p < shared:
            t_copy(p).start()

    start = 0
    for i, size in enumerate(T_BLOCKS):
        ps = range(start, start + size)
        start += size
        for p in ps:
            b_copy(p).wait()
        if i == 0:
            for p in range(T_BLOCKS[0] + T_BLOCKS[1], pairs):
                b_copy(p).start()
        for p in ps:
            t_step(p)
        if i == 0:
            pl.semaphore_wait(barrier, 10)
        for p in ps:
            send_t(p)

    def take(s):
        for j in range(shared):
            for e in range(2):
                for k, part in enumerate(split3(t_r[j, e, :, s * 128:(s + 1) * 128])):
                    oth[s, j, k, e] = part

    def coulomb(ps, cols, width, old=None):
        qs = [(p, e) for p in ps for e in range(2)]
        g = [jnp.sum(g_f[q] + g_r[q]) for q in qs]
        out = []
        for row in range(0, half, 8):
            total = None if old is None else old[row:row + 8, :]
            for gq, (p, e) in zip(g, qs):
                term = gq * b_v[2 * p + e, row:row + 8, pl.ds(cols, width)]
                total = term if total is None else total + term
            out.append(total)
        return jnp.concatenate(out, axis=0)

    def own_sum(s, ps):
        total = None
        for p in ps:
            wh, wm, wl = (joined(own.at[p, k, s]) for k in range(3))
            term = mm_nt(wh * 0.5, wh) + mm_nt(wm, wh) + mm_nt(wl, wh) + mm_nt(wm * 0.5, wm)
            total = term if total is None else total + term
        return total

    def oth_sum(s, work):
        total = None
        for j, parts in work:
            for k in parts:
                right = joined(own.at[shared + j, k, s])
                for lhs in range(3 - k):
                    term = mm_nt(joined(oth.at[s, j, lhs]), right)
                    total = term if total is None else total + term
        return total

    def own_products(s):
        return own_sum(s, range(pairs))

    def oth_products(s):
        return oth_sum(s, [(j, (0, 1, 2)) for j in range(shared)])

    def block(body):
        def trip(_, carry):
            body()
            return carry
        lax.fori_loop(orb, orb + 1, trip, 0)

    z_pair = (pl.ds(2 * orb, 2), pl.ds(2 * (1 - orb), 2))

    def put(s, part, block):
        for h in range(2):
            p_buf[s, h, z_pair[part]] = block[:, h * 128:(h + 1) * 128].reshape(2, 4, 4, 8, 128)

    def put_oth(s):
        put(s, 1, -(z_f[s] + z_r[s]))

    def by_core(body, *args):
        for r in range(2):
            @pl.when(orb == r)
            def _():
                body(r, *args)

    dists = (2, 1, 3)

    def line1(axis, zs, where):
        return {0: (where,), 1: (zs, where), 2: (zs, slice(None), where)}[axis]

    def copy1(r, s, h, part, dist):
        axis = ORDERS[r][s][h][0]
        zs = pl.ds(2 * (r if part == 0 else 1 - r), 2)
        device, target = peer(axis, dist)
        dst = r1.at[s, h, dist - 1] if axis == 0 else r1.at[s, h, dist - 1, zs]
        return pltpu.make_async_remote_copy(
            src_ref=p_buf.at[(s, h) + line1(axis, zs, target)], dst_ref=dst,
            send_sem=send1.at[s, h, part, dist - 1], recv_sem=recv1.at[s, h, part, dist - 1],
            device_id=device, device_id_type=MESH)

    def copy2(r, s, h, dist):
        order = ORDERS[r][s][h]
        device, target = peer(order[1], dist)
        where = (target,) if order[1] == min(order[1:]) else (slice(None), target)
        return pltpu.make_async_remote_copy(
            src_ref=s1.at[(s, h) + where], dst_ref=r2.at[s, h, dist - 1],
            send_sem=send2.at[s, h, dist - 1], recv_sem=recv2.at[s, h, dist - 1],
            device_id=device, device_id_type=MESH)

    def copy3(r, s, h, dist):
        device, target = peer(ORDERS[r][s][h][2], dist)
        return pltpu.make_async_remote_copy(
            src_ref=s2.at[s, h, target], dst_ref=r3.at[s, h, dist - 1],
            send_sem=send3.at[s, h, dist - 1], recv_sem=recv3.at[s, h, dist - 1],
            device_id=device, device_id_type=MESH)

    def start1(r, s, part):
        for dist in dists:
            for h in range(2):
                if ORDERS[r][s][h][0] == 0:
                    @pl.when((peer(0, dist)[1] // 2 == r) == (part == 0))
                    def _():
                        copy1(r, s, h, 0, dist).start()
                else:
                    copy1(r, s, h, part, dist).start()

    def parts1(r, s, h):
        return (0,) if ORDERS[r][s][h][0] == 0 else (1, 0)

    def finish1(r, s):
        for h in range(2):
            axis = ORDERS[r][s][h][0]
            for part in parts1(r, s, h):
                for dist in dists:
                    copy1(r, s, h, part, dist).wait_recv()
                zs = pl.ds(2 * (r if part == 0 else 1 - r), 2)
                kept = p_buf[(s, h) + line1(axis, zs, coords[axis])]
                if axis == 0:
                    s1[s, h] = kept + r1[s, h, 0] + r1[s, h, 1] + r1[s, h, 2]
                else:
                    s1[s, h, zs] = kept + r1[s, h, 0, zs] + r1[s, h, 1, zs] + r1[s, h, 2, zs]
            for dist in dists:
                copy2(r, s, h, dist).start()

    def finish2(r, s):
        for h in range(2):
            order = ORDERS[r][s][h]
            for dist in dists:
                copy2(r, s, h, dist).wait_recv()
            where = (coords[order[1]],) if order[1] == min(order[1:]) else (slice(None), coords[order[1]])
            s2[s, h] = s1[(s, h) + where] + r2[s, h, 0] + r2[s, h, 1] + r2[s, h, 2]
            for dist in dists:
                copy3(r, s, h, dist).start()

    def finish3(r, s):
        for h in range(2):
            for dist in dists:
                copy3(r, s, h, dist).wait_recv()
            o_ref[s, :, h * 128:(h + 1) * 128] = (
                s2[s, h, coords[ORDERS[r][s][h][2]]] + r3[s, h, 0] + r3[s, h, 1] + r3[s, h, 2])

    def sent(r, s, phase):
        for h in range(2):
            for dist in dists:
                if phase == 0:
                    for part in parts1(r, s, h):
                        copy1(r, s, h, part, dist).wait_send()
                else:
                    (copy2, copy3)[phase - 1](r, s, h, dist).wait_send()

    def reduce_rest(r):
        for phase, finish in enumerate((finish1, finish2, finish3)):
            if phase == 2:
                for s in range(2):
                    sent(r, s, 2)
            for s in range(2):
                finish(r, s)
                if phase < 2:
                    sent(r, s, phase)

    kept = range(shared, pairs)

    def alpha_oth():
        take(0)
        j_t[...] = coulomb(kept, oth_row, half).T
        j_acc[...] = coulomb(kept, own_row, half)
        z = oth_products(0) - j_t[...]
        z_f[0] = z
        z_t[0] = z.T

    def beta_oth():
        take(1)
        j_acc[...] = coulomb(range(shared), own_row, half, j_acc)
        z = oth_products(1) - j_t[...]
        z_f[1] = z
        z_t[1] = z.T

    def own_block(s):
        y = own_products(s)
        put(s, 0, j_acc[...] - (y + y.T))

    for p in range(shared):
        t_copy(p).wait_recv()
        g_landed(shared + p)
    block(alpha_oth)
    z_copy(0).start()
    for p in range(shared):
        g_landed(p)
    block(beta_oth)
    z_copy(1).start()
    z_copy(0).wait_recv()
    put_oth(0)
    by_core(start1, 0, 1)
    block(functools.partial(own_block, 0))
    by_core(start1, 0, 0)
    z_copy(1).wait_recv()
    put_oth(1)
    by_core(start1, 1, 1)
    block(functools.partial(own_block, 1))
    by_core(start1, 1, 0)
    for p in range(shared):
        t_copy(p).wait_send()
    for p in range(pairs):
        g_copy(p).wait_send()
    for s in range(2):
        z_copy(s).wait_send()
    by_core(reduce_rest)


def solution(mesh):
    def local_build(b_local, c_alpha, c_beta):
        n_q, half, rows = b_local.shape
        pairs = n_q // 2
        vmem = pltpu.VMEM
        dma = pltpu.SemaphoreType.DMA
        anywhere = pl.BlockSpec(memory_space=pl.ANY)
        out = pl.pallas_call(
            functools.partial(kernel, n_q, rows),
            out_shape=pltpu.VMEM((2, 8, half), F32),
            in_specs=[anywhere, anywhere, anywhere],
            out_specs=pl.BlockSpec(memory_space=vmem),
            scratch_shapes=[
                vmem((n_q, half, rows), F32),
                vmem((c_alpha.shape[1], rows), F32),
                vmem((c_beta.shape[1], rows), F32),
                vmem((256, rows), F32),
                vmem((rows, 256), F32),
                vmem((3, 2, rows, 128), BF16),
                vmem((pairs, 2, half, 256), F32),
                vmem((pairs // 2, 2, half, 256), F32),
                vmem((pairs, 2, 8, 128), F32),
                vmem((pairs, 2, 8, 128), F32),
                vmem((pairs, 3, 2, 2, half, 128), BF16),
                vmem((2, pairs // 2, 3, 2, half, 128), BF16),
                vmem((half, half), F32),
                vmem((half, half), F32),
                vmem((2, half, half), F32),
                vmem((2, half, half), F32),
                vmem((2, half, half), F32),
                vmem((2, 2, 4, 4, 4, 8, 128), F32),
                vmem((2, 2, 3, 4, 4, 8, 128), F32),
                vmem((2, 2, 4, 4, 8, 128), F32),
                vmem((2, 2, 3, 4, 8, 128), F32),
                vmem((2, 2, 4, 8, 128), F32),
                vmem((2, 2, 3, 8, 128), F32),
                dma((pairs,)),
                dma((2,)),
                dma((pairs // 2,)),
                dma((pairs // 2,)),
                dma((pairs,)),
                dma((pairs,)),
                dma((2,)),
                dma((2,)),
                dma((2, 2, 2, 3)),
                dma((2, 2, 2, 3)),
                dma((2, 2, 3)),
                dma((2, 2, 3)),
                dma((2, 2, 3)),
                dma((2, 2, 3)),
            ],
            compiler_params=pltpu.CompilerParams(
                collective_id=0, has_side_effects=True, vmem_limit_bytes=60 * 1024 * 1024),
        )(b_local, c_alpha.T, c_beta.T)
        return out[0].T, out[1].T

    spec_b = P(("sys", "aux"), "orb", None)
    spec_c = P("sys", None)
    spec_g = P(("sys", "orb"), "aux")
    return jax.shard_map(local_build, mesh=mesh, in_specs=(spec_b, spec_c, spec_c), out_specs=(spec_g, spec_g), check_vma=False)
```
